128 devices in a mesh: band: 32 (over z, y_hi, x), gvec: 4 (over y_lo, core).
Axes of the slice: x: 4, y: 4 (y_hi: 2, y_lo: 2; y = y_hi * 2 + y_lo), z: 4, core: 2. Of those that a mesh axis runs over, the one named last changes fastest.
Arguments:
- wave_coeffs: bfloat16 [2, 1024, 75264], P(None, 'band', 'gvec'), may hold values from -6 to 6
- projectors: bfloat16 [2, 256, 75264], P(None, 'band', 'gvec'), may hold values from -0.0234375 to 0.0234375
- miller_index: int32 [3, 75264], P(None, 'gvec'), may hold values from -24 to 24
- lattice: float32 [3, 3], replicated, may hold values from -0.25 to 1.25
- occupation: float32 [1024], P('band'), may hold values from 0 to 2
- species: int32 [32], replicated, may hold values from 0 to 3
- proj_count: int32 [32], replicated, may hold values from 4 to 8
- coupling: float32 [4, 8, 8], replicated, may hold values from -0.4 to 2, as said below
Outputs:
- forces: float32 [3, 32], P(None, 'band')
- stress: float32 [3, 3], replicated
The draws below stay inside these ranges and needn't reach their ends.
Inputs may be any that keep to these rules, and one draw needn't show every extreme that they name: `coupling`: symmetric in its last two dimensions.
All inputs are finite; a program needn't handle non-finite values.
Results may differ from the reference program's by a relative error of at most 0.006.
Values may be sent and summed in bfloat16 or wider, within the bound.
A program may use at most 64 MiB of HBM per device.

```python
import math
import jax
import jax.numpy as jnp
from jax import lax

NG = 75264
PROJ = 8
NSPEC = 4
MILLER = 24
NATOMS = 32
NPROJ = 256
NBANDS = 1024


def draw_lattice(key, part):
    spread = 0.15
    noise = jax.random.uniform(key, (3, 3), jnp.float32, -spread, spread)
    return jnp.eye(3, dtype=jnp.float32) + noise


def draw_occupation(key, part):
    center_key, width_key = jax.random.split(key)
    center = jax.random.uniform(center_key, (), jnp.float32, 0.4, 0.75) * NBANDS
    spread = jax.random.uniform(width_key, (), jnp.float32, 0.08, 0.15) * NBANDS
    position = jnp.arange(NBANDS, dtype=jnp.float32)
    return 2.0 / (1.0 + jnp.exp((position - center) / spread))


def draw_coupling(key, part):
    diag_key, off_key = jax.random.split(key)
    diagonal = jax.random.uniform(diag_key, (NSPEC, PROJ), jnp.float32, 0.5, 2.0)
    off_values = jax.random.uniform(off_key, (NSPEC, PROJ, PROJ), jnp.float32, -0.4, 0.4)
    symmetric = 0.5 * (off_values + jnp.swapaxes(off_values, 1, 2))
    identity = jnp.eye(PROJ, dtype=jnp.float32)
    return symmetric * (1.0 - identity) + diagonal[:, :, None] * identity


def set_ends(values, stream_key, low, largest):
    dims = values.shape
    place = [jax.random.randint(jax.random.fold_in(stream_key, axis), (), 0, dims[axis]) for axis in range(len(dims))]
    values = values.at[tuple(place)].set(low)
    longest = dims.index(max(dims))
    place[longest] = (place[longest] + 1) % dims[longest]
    return values.at[tuple(place)].set(largest)


def level_of(own_key, extent, cuts, low, high):
    factor_of, own = 1.0, jax.random.fold_in(own_key, 6)
    for axis_at, shards_of in cuts:
        draws = jnp.exp(jax.random.uniform(jax.random.fold_in(own, axis_at), (shards_of,), jnp.float32, low / len(cuts), high / len(cuts)))
        factor_of = factor_of * jnp.repeat(draws, extent[axis_at] // shards_of).reshape([-1 if axis == axis_at else 1 for axis in range(len(extent))])
    return factor_of


def bell_draw(own_key, dims, scale, bound, cuts=(), kind=jnp.bfloat16):
    values = scale * jax.random.normal(own_key, dims, jnp.float32)
    if cuts:
        values = values * level_of(own_key, dims, cuts, -0.22, 0.18)
    return jnp.clip(values, -bound, bound).astype(kind)


def setup_inputs(seed: int = 0) -> dict:
    keys = jax.random.split(jax.random.key(seed), 9)
    wave_coeffs = bell_draw(keys[0], (2, NBANDS, NG), 1.0, 6.0, ((1, 32), (2, 4)))
    projectors = bell_draw(keys[1], (2, NPROJ, NG), NG ** -0.5, 0.0234375, ((1, 32), (2, 4)))
    miller_index = set_ends(jax.random.randint(keys[2], (3, NG), -MILLER, MILLER + 1), jax.random.fold_in(keys[2], 1), -MILLER, MILLER).astype(jnp.int32)
    lattice = draw_lattice(jax.random.fold_in(keys[8], 71), 0)
    occupation = draw_occupation(jax.random.fold_in(keys[8], 71), 0)
    species = set_ends(jax.random.randint(keys[5], (NATOMS,), 0, NSPEC), jax.random.fold_in(keys[5], 1), 0, NSPEC - 1).astype(jnp.int32)
    proj_count = set_ends(jax.random.randint(keys[6], (NATOMS,), PROJ // 2, PROJ + 1), jax.random.fold_in(keys[6], 1), PROJ // 2, PROJ).astype(jnp.int32)
    coupling = draw_coupling(jax.random.fold_in(keys[8], 71), 0)
    return dict(wave_coeffs=wave_coeffs, projectors=projectors, miller_index=miller_index, lattice=lattice, occupation=occupation, species=species, proj_count=proj_count, coupling=coupling)


stress_pairs = ((0, 0), (1, 1), (2, 2), (0, 1), (0, 2), (1, 2))

def cart_weights(miller_index, lattice):
    indices = miller_index.astype(jnp.float32)
    coords = []
    for column in range(3):
        coords.append((indices[0] * lattice[0, column] + indices[1] * lattice[1, column] + indices[2] * lattice[2, column]) / MILLER)
    isotropic = (coords[0] * coords[0] + coords[1] * coords[1] + coords[2] * coords[2]) / 3.0
    weight_rows = [jnp.ones_like(coords[0])] + coords
    for first_axis, second_axis in stress_pairs:
        product = coords[first_axis] * coords[second_axis]
        if first_axis == second_axis:
            product = product - isotropic
        weight_rows.append(product)
    return jnp.stack(weight_rows)

def scale_block(weights, atom_block):
    proj_rows = atom_block.shape[1]
    scaled = (weights[:, None, None, :] * atom_block[None].astype(jnp.float32)).astype(jnp.bfloat16)
    return scaled.reshape(20 * proj_rows, atom_block.shape[2])

def intersection(scaled, flat_waves):
    product = lax.dot_general(scaled, flat_waves, (((1,), (1,)), ((), ())), preferred_element_type=jnp.float32)
    product = product.reshape(10, 2, scaled.shape[0] // 20, 2, flat_waves.shape[0] // 2)
    real_part = product[:, 0, :, 0] + product[:, 1, :, 1]
    imag_part = product[:, 0, :, 1] - product[:, 1, :, 0]
    return jnp.stack([real_part, imag_part], axis=1)

def atom_couplings(species, proj_count, coupling):
    kind_count = coupling.shape[0]
    proj_width = coupling.shape[1]
    onehot = (species[:, None] == jnp.arange(kind_count, dtype=jnp.int32)[None, :]).astype(jnp.float32)
    chosen = jnp.einsum('as,sij->aij', onehot, coupling, precision=lax.Precision.HIGHEST)
    active = (jnp.arange(proj_width, dtype=jnp.int32)[None, :] < proj_count[:, None]).astype(jnp.float32)
    return chosen * active[:, :, None] * active[:, None, :]

def contract(per_atom, couplings, occupied):
    mixed = jnp.einsum('aij,kcajn->kcain', couplings, per_atom, precision=lax.Precision.HIGHEST)
    becp_real = per_atom[0, 0]
    becp_imag = per_atom[0, 1]
    imag_sum = lax.optimization_barrier(jnp.sum(becp_real[None] * mixed[1:4, 1] - becp_imag[None] * mixed[1:4, 0], axis=2))
    real_sum = lax.optimization_barrier(jnp.sum(becp_real[None] * mixed[4:, 0] + becp_imag[None] * mixed[4:, 1], axis=2))
    force_part = lax.optimization_barrier(jnp.sum(imag_sum * occupied, axis=2))
    stress_part = lax.optimization_barrier(jnp.sum(real_sum * occupied, axis=(1, 2)))
    return (force_part, stress_part)

def stress_matrix(values):
    return jnp.stack([jnp.stack([values[0], values[3], values[4]]), jnp.stack([values[3], values[1], values[5]]), jnp.stack([values[4], values[5], values[2]])])

def reference(wave_coeffs, projectors, miller_index, lattice, occupation, species, proj_count, coupling):
    weights = cart_weights(miller_index, lattice)
    flat_waves = wave_coeffs.reshape(2 * NBANDS, NG)
    atom_blocks = projectors.reshape(2, NATOMS, PROJ, NG).transpose(1, 0, 2, 3)
    intersections = lax.map(lambda atom_block: intersection(scale_block(weights, atom_block), flat_waves), atom_blocks)
    per_atom = intersections.transpose(1, 2, 0, 3, 4)
    force_part, stress_part = contract(per_atom, atom_couplings(species, proj_count, coupling), occupation)
    force_scale = 2.0 / (PROJ * math.sqrt(NBANDS))
    stress_scale = 1.0 / (PROJ * math.sqrt(NATOMS * NBANDS))
    return (force_part * force_scale, stress_matrix(stress_part * stress_scale))
```

```python
import functools
import math

import jax
import jax.numpy as jnp
from jax import lax
from jax.experimental import pallas as pl
from jax.experimental.pallas import tpu as pltpu
from jax.sharding import Mesh
from jax.sharding import PartitionSpec as P

PROJ = 8
MILLER = 24.0
LANE = 128
MESH = pl.DeviceIdType.MESH
F32 = jnp.float32
BF16 = jnp.bfloat16
AXES = ("z", "yh", "x", "yl", "core")


def kernel(
    dims, nt, tiles, chunks, scales,
    psi_hbm, proj_hbm, miller_hbm, lat_ref, occ_ref, spec_ref, cnt_ref, coup_ref,
    force_ref, stress_ref,
    psi_buf, p_buf, mil_buf, occ_buf, w_buf, acc, b_send, rs_buf, uv_buf, negv, facc, sacc, tot_a, tot_b,
    loc_sem, psend, precv, zsend, zrecv, ssend, srecv, osend, orecv, rsend, rrecv, asend, arecv, fsend, frecv, gsend, grecv,
):
    nz, nyh, nx, nyl, nc = dims
    n_s = nyh * nx
    n_r = n_s * nyl * nc
    z, yh, x, yl, c = (lax.axis_index(a) for a in AXES)
    me_s = yh * nx + x
    me_r = me_s * (nyl * nc) + yl * nc + c
    beta = z * n_s + me_s
    n_chunk = len(chunks)

    def s_peer(k):
        q = lax.rem(me_s + k, n_s)
        return q, {"yh": q // nx, "x": lax.rem(q, nx)}

    def r_peer(k):
        r = lax.rem(me_r + k, n_r)
        q = r // (nyl * nc)
        rest = lax.rem(r, nyl * nc)
        return r, {"yh": q // nx, "x": lax.rem(q, nx), "yl": rest // nc, "core": lax.rem(rest, nc)}

    def z_peer(k):
        return {"z": lax.rem(z + k, nz)}

    def first_tile(q):
        return (q * tiles) // n_s

    def remote(src, dst, ssem, rsem, where):
        return pltpu.make_async_remote_copy(src, dst, ssem, rsem, device_id=where, device_id_type=MESH)

    def wait_recv(ref, sem):
        remote(ref, ref, sem, sem, s_peer(1)[1]).wait_recv()

    def wait_send(ref, sem):
        remote(ref, ref, sem, sem, s_peer(1)[1]).wait_send()

    my_off = first_tile(me_s) * LANE

    def local_copies():
        out = [pltpu.make_async_copy(miller_hbm.at[:, pl.ds(pl.multiple_of(my_off, LANE), nt * LANE)], mil_buf.at[:, pl.ds(0, nt * LANE)], loc_sem.at[0])]
        out.append(pltpu.make_async_copy(
            proj_hbm.at[:, :, pl.ds(pl.multiple_of(my_off, LANE), nt * LANE)],
            p_buf.at[:, beta, :, pl.ds(0, nt * LANE)], loc_sem.at[1]))
        out.append(pltpu.make_async_copy(
            psi_hbm.at[:, :, pl.ds(pl.multiple_of(my_off, LANE), nt * LANE)],
            psi_buf.at[:, pl.ds(pl.multiple_of(me_s * 32, 32), 32), pl.ds(0, nt * LANE)], loc_sem.at[2]))
        return out

    for cp in local_copies():
        cp.start()

    bar = pltpu.get_barrier_semaphore()

    def hello(k, carry):
        _, where = r_peer(k)
        pl.semaphore_signal(bar, 1, device_id=where, device_id_type=MESH)
        return carry

    lax.fori_loop(1, n_r, hello, 0)
    for k in range(1, nz):
        pl.semaphore_signal(bar, 1, device_id=z_peer(k), device_id_type=MESH)
    pl.semaphore_wait(bar, n_r - 1 + nz - 1)

    for i, (t0, tn) in enumerate(chunks):
        for k in range(1, n_s):
            q, where = s_peer(k)
            off = pl.multiple_of((first_tile(q) + t0) * LANE, LANE)
            remote(proj_hbm.at[:, :, pl.ds(off, tn * LANE)],
                   p_buf.at[:, beta, :, pl.ds(t0 * LANE, tn * LANE)], psend, precv.at[i], where).start()
    for k in range(1, n_s):
        q, where = s_peer(k)
        remote(occ_ref, occ_buf.at[me_s], osend, orecv, where).start()
    for i, (t0, tn) in enumerate(chunks):
        for k in range(1, n_s):
            q, where = s_peer(k)
            off = pl.multiple_of((first_tile(q) + t0) * LANE, LANE)
            remote(psi_hbm.at[:, :, pl.ds(off, tn * LANE)],
                   psi_buf.at[:, pl.ds(pl.multiple_of(me_s * 32, 32), 32), pl.ds(t0 * LANE, tn * LANE)], ssend, srecv.at[i], where).start()

    local = local_copies()
    local[0].wait()
    kp = w_buf.shape[1]
    used = nt * LANE
    if kp > used:
        pad = kp - used
        mil_buf[:, pl.ds(used, pad)] = jnp.zeros((3, pad), jnp.int32)
        psi_buf[:, :, pl.ds(used, pad)] = jnp.zeros((2, psi_buf.shape[1], pad), BF16)
        p_buf[:, :, :, pl.ds(used, pad)] = jnp.zeros((2, p_buf.shape[1], PROJ, pad), BF16)
    own_tiles = first_tile(me_s + 1) - first_tile(me_s)
    valid = (lax.broadcasted_iota(jnp.int32, (1, kp), 1) < own_tiles * LANE).astype(F32)
    idx = [mil_buf[a : a + 1, :].astype(F32) for a in range(3)]
    co = [(idx[0] * lat_ref[0, a] + idx[1] * lat_ref[1, a] + idx[2] * lat_ref[2, a]) / MILLER for a in range(3)]
    iso = (co[0] * co[0] + co[1] * co[1] + co[2] * co[2]) / 3.0
    rows = list(co)
    for a, b in ((0, 0), (1, 1), (2, 2), (0, 1), (0, 2), (1, 2)):
        prod = co[a] * co[b]
        rows.append(prod - iso if a == b else prod)
    for m, row in enumerate(rows):
        w_buf[m : m + 1, :] = row * valid
    facc[...] = jnp.zeros_like(facc)
    sacc[...] = jnp.zeros_like(sacc)
    acc[...] = jnp.zeros_like(acc)

    local[1].wait()
    plane = pl.ds(pl.multiple_of(z * n_s, n_s), n_s)
    for i, (t0, tn) in enumerate(chunks):
        part = pl.ds(t0 * LANE, tn * LANE)
        wait_recv(p_buf.at[:, pl.ds(0, n_s - 1), :, part], precv.at[i])
        for k in range(1, nz):
            remote(p_buf.at[:, plane, :, part], p_buf.at[:, plane, :, part], zsend, zrecv.at[i], z_peer(k)).start()

    local[2].wait()
    nb = psi_buf.shape[1]
    na = p_buf.shape[1]
    for i, (t0, tn) in enumerate(chunks):
        part = pl.ds(t0 * LANE, tn * LANE)
        wait_recv(p_buf.at[:, pl.ds(0, n_s * (nz - 1)), :, part], zrecv.at[i])
        wait_recv(psi_buf.at[:, pl.ds(0, 32 * (n_s - 1)), part], srecv.at[i])
        rhs = psi_buf[:, :, part].reshape(2 * nb, tn * LANE)
        lhs = p_buf[:, :, :, part].reshape(2 * na * PROJ, tn * LANE)
        if i == n_chunk - 1:
            keep = (lax.broadcasted_iota(jnp.int32, (1, tn * LANE), 1) + t0 * LANE < own_tiles * LANE)
            lhs = jnp.where(keep, lhs, jnp.zeros_like(lhs))
        acc[...] += lax.dot_general(lhs, rhs, (((1,), (1,)), ((), ())), preferred_element_type=F32)

    np_ = na * PROJ
    b_send[:, 0] = (acc[:np_, :nb] + acc[np_:, nb:]).reshape(na, PROJ, nb).astype(BF16)
    b_send[:, 1] = (acc[:np_, nb:] - acc[np_:, :nb]).reshape(na, PROJ, nb).astype(BF16)

    def give(k, carry):
        r, where = r_peer(k)
        remote(b_send.at[r], rs_buf.at[me_r], rsend, rrecv, where).start()
        return carry

    lax.fori_loop(1, n_r, give, 0)
    rs_buf[me_r] = b_send[me_r]
    wait_recv(occ_buf.at[pl.ds(0, n_s - 1)], orecv)
    occ_buf[me_s] = occ_ref[...]
    occ = jnp.sum(occ_buf[...], axis=0)
    kind = spec_ref[me_r]
    count = cnt_ref[me_r]
    mat = coup_ref[kind]
    act = (lax.broadcasted_iota(jnp.int32, (PROJ, PROJ), 0) < count) & (lax.broadcasted_iota(jnp.int32, (PROJ, PROJ), 1) < count)
    mat = jnp.where(act, mat, 0.0)
    wait_recv(rs_buf.at[pl.ds(0, n_r - 1)], rrecv)
    total = jnp.sum(rs_buf[...].astype(F32), axis=0)
    for h in range(2):
        mixed = jnp.zeros((PROJ, nb), F32)
        for i in range(PROJ):
            mixed = mixed + mat[:, i : i + 1] * total[h, i : i + 1, :]
        uv_buf[h, me_r] = (mixed * occ).astype(BF16)

    def spread(k, carry):
        _, where = r_peer(k)
        remote(uv_buf.at[:, me_r], uv_buf.at[:, me_r], asend, arecv, where).start()
        return carry

    lax.fori_loop(1, n_r, spread, 0)
    wait_recv(uv_buf.at[:, pl.ds(0, n_r - 1)], arecv)

    u = uv_buf[0].reshape(np_, nb)
    v = uv_buf[1].reshape(np_, nb)
    negv[0] = u
    negv[1] = v
    negv[2] = -v

    wide = 256

    def block(i, carry):
        cols = pl.ds(pl.multiple_of(i * wide, wide), wide)
        re = psi_buf[0, :, cols]
        im = psi_buf[1, :, cols]
        dot = functools.partial(jnp.dot, preferred_element_type=F32)
        y_re = dot(negv[0], re) + dot(negv[1], im)
        y_im = dot(negv[0], im) + dot(negv[2], re)
        p_re = p_buf[0, :, :, cols].astype(F32).reshape(np_, wide)
        p_im = p_buf[1, :, :, cols].astype(F32).reshape(np_, wide)
        e_im = (p_re * y_im - p_im * y_re).reshape(na, PROJ, wide)
        e_re = jnp.sum((p_re * y_re + p_im * y_im).reshape(na, PROJ, wide), axis=0)
        for a in range(3):
            t = e_im * w_buf[a : a + 1, cols].reshape(1, 1, wide)
            facc[a] += t[:, :, :LANE] + t[:, :, LANE:]
        for m in range(6):
            t = e_re * w_buf[3 + m : 4 + m, cols]
            sacc[m] += t[:, :LANE] + t[:, LANE:]
        return carry

    lax.fori_loop(0, kp // wide, block, 0)

    out_rows = []
    for a in range(3):
        f = jnp.sum(facc[a], axis=1)
        if na < LANE:
            f = jnp.concatenate([f, jnp.zeros((LANE - na, LANE), F32)], axis=0)
        out_rows.append(jnp.sum(f.T, axis=0, keepdims=True))
    lane = lax.broadcasted_iota(jnp.int32, (1, LANE), 1)
    srow = jnp.zeros((1, LANE), F32)
    for m in range(6):
        srow = srow + jnp.where(lane == m, jnp.sum(sacc[m], keepdims=True), 0.0)
    mine = jnp.concatenate(out_rows + [srow] + [jnp.zeros((4, LANE), F32)], axis=0)
    tot_a[me_r] = mine

    def share(k, carry):
        _, where = r_peer(k)
        remote(tot_a.at[me_r], tot_a.at[me_r], fsend, frecv, where).start()
        return carry

    lax.fori_loop(1, n_r, share, 0)
    wait_recv(tot_a.at[pl.ds(0, n_r - 1)], frecv)
    tot_b[z] = jnp.sum(tot_a[...], axis=0)
    for k in range(1, nz):
        remote(tot_b.at[z], tot_b.at[z], gsend, grecv, z_peer(k)).start()
    wait_recv(tot_b.at[pl.ds(0, nz - 1)], grecv)
    res = jnp.sum(tot_b[...], axis=0)
    force_ref[...] = jnp.sum(jnp.where(lane == beta, res[0:3, :], 0.0), axis=1, keepdims=True) * scales[0]
    i0 = lax.broadcasted_iota(jnp.int32, (3, 3), 0)
    i1 = lax.broadcasted_iota(jnp.int32, (3, 3), 1)
    st = jnp.zeros((3, 3), F32)
    for m, (a, b) in enumerate(((0, 0), (1, 1), (2, 2), (0, 1), (0, 2), (1, 2))):
        val = jnp.sum(jnp.where(lane == m, res[3:4, :], 0.0), axis=1, keepdims=True)
        hit = ((i0 == a) & (i1 == b)) | ((i0 == b) & (i1 == a))
        st = st + jnp.where(hit, val, 0.0)
    stress_ref[...] = st * scales[1]

    for i, (t0, tn) in enumerate(chunks):
        part = pl.ds(t0 * LANE, tn * LANE)
        wait_send(p_buf.at[:, pl.ds(0, n_s - 1), :, part], psend)
        wait_send(psi_buf.at[:, pl.ds(0, 32 * (n_s - 1)), part], ssend)
        wait_send(p_buf.at[:, pl.ds(0, n_s * (nz - 1)), :, part], zsend)
    wait_send(occ_buf.at[pl.ds(0, n_s - 1)], osend)
    wait_send(rs_buf.at[pl.ds(0, n_r - 1)], rsend)
    wait_send(uv_buf.at[:, pl.ds(0, n_r - 1)], asend)
    wait_send(tot_a.at[pl.ds(0, n_r - 1)], fsend)
    wait_send(tot_b.at[pl.ds(0, nz - 1)], gsend)


def body(dims, psi, proj, miller, lattice, occupation, species, proj_count, coupling):
    nz, nyh, nx, nyl, nc = dims
    n_s = nyh * nx
    n_r = n_s * nyl * nc
    bands = psi.shape[1]
    tiles = psi.shape[2] // LANE
    atoms = species.shape[0]
    nt = -(-tiles // n_s)
    sizes = []
    left = nt
    for want in (6, 6, 4):
        if left > want:
            sizes.append(want)
            left -= want
    sizes.append(left)
    chunks, at = [], 0
    for n in sizes:
        chunks.append((at, n))
        at += n
    kp = -(-nt * LANE // 256) * 256
    nb = n_s * bands
    me_s = lax.axis_index("yh") * nx + lax.axis_index("x")
    zero = jnp.zeros((), jnp.int32)
    occ_row = lax.dynamic_update_slice(jnp.zeros((1, nb), F32), occupation[None], (zero, me_s * bands))
    band_total = nb * nz
    scales = (2.0 / (PROJ * math.sqrt(band_total)), 1.0 / (PROJ * math.sqrt(atoms * band_total)))
    any_spec = pl.BlockSpec(memory_space=pl.ANY)
    vmem = pl.BlockSpec(memory_space=pltpu.VMEM)
    smem = pl.BlockSpec(memory_space=pltpu.SMEM)
    dma = pltpu.SemaphoreType.DMA
    nch = len(chunks)
    return pl.pallas_call(
        functools.partial(kernel, dims, nt, tiles, tuple(chunks), scales),
        out_shape=(jax.ShapeDtypeStruct((3, 1), F32), jax.ShapeDtypeStruct((3, 3), F32)),
        in_specs=[any_spec, any_spec, any_spec, smem, vmem, smem, smem, vmem],
        out_specs=(vmem, vmem),
        scratch_shapes=[
            pltpu.VMEM((2, nb, kp), BF16),
            pltpu.VMEM((2, atoms, PROJ, kp), BF16),
            pltpu.VMEM((3, kp), jnp.int32),
            pltpu.VMEM((n_s, 1, nb), F32),
            pltpu.VMEM((16, kp), F32),
            pltpu.VMEM((2 * atoms * PROJ, 2 * nb), F32),
            pltpu.VMEM((atoms, 2, PROJ, nb), BF16),
            pltpu.VMEM((n_r, 2, PROJ, nb), BF16),
            pltpu.VMEM((2, n_r, PROJ, nb), BF16),
            pltpu.VMEM((3, atoms * PROJ, nb), BF16),
            pltpu.VMEM((3, atoms, PROJ, LANE), F32),
            pltpu.VMEM((6, PROJ, LANE), F32),
            pltpu.VMEM((n_r, 8, LANE), F32),
            pltpu.VMEM((nz, 8, LANE), F32),
            dma((3,)), dma, dma((nch,)), dma, dma((nch,)), dma, dma((nch,)), dma, dma, dma, dma, dma, dma, dma, dma, dma, dma,
        ],
        compiler_params=pltpu.CompilerParams(collective_id=0, has_side_effects=True, vmem_limit_bytes=58 << 20),
        name="plane_kernel",
    )(psi, proj, miller, lattice, occ_row, species, proj_count, coupling)


def solution(mesh, dims=(4, 2, 4, 2, 2)):
    finer = Mesh(mesh.devices.reshape(dims), AXES)
    band, gvec = ("z", "yh", "x"), ("yl", "core")
    in_specs = (P(None, band, gvec), P(None, band, gvec), P(None, gvec), P(), P(band), P(), P(), P())
    return jax.shard_map(functools.partial(body, dims), mesh=finer, in_specs=in_specs, out_specs=(P(None, band), P()), check_vma=False)
```

```python
import functools
import itertools
import math

import jax
import jax.numpy as jnp
from jax import lax
from jax.experimental import pallas as pl
from jax.experimental.pallas import tpu as pltpu
from jax.sharding import Mesh
from jax.sharding import PartitionSpec as P

PROJ = 8
MILLER = 24.0
LANE = 128
LOGICAL = pl.DeviceIdType.LOGICAL
F32 = jnp.float32
BF16 = jnp.bfloat16
AXES = ("z", "yh", "x", "yl", "core")


def kernel(
    dims, nt, tiles, chunks,
    psi_hbm, proj_hbm, miller_hbm, lat_hbm, occ_hbm, spec_hbm, cnt_hbm, coup_hbm,
    out_ref,
    psi_buf, p_buf, mil_buf, occ_buf, w_buf, acc, b_send, rs_buf, uv_buf, negv, facc, sacc, tot,
    lat_ref, spec_ref, cnt_ref, coup_ref, occ_row, occ_in,
    loc_sem, psend, precv, zsend, zrecv, ssend, srecv, osend, orecv, rsend, rrecv, asend, arecv, fsend, frecv,
):
    nz, nyh, nx, nyl, nc = dims
    n_s = nyh * nx
    n_r = n_s * nyl * nc
    z, yh, x, yl, c = (lax.axis_index(a) for a in AXES)
    me_s = yh * nx + x
    me_r = me_s * (nyl * nc) + yl * nc + c
    beta = z * n_s + me_s
    n_chunk = len(chunks)

    n_all = nz * n_r
    me = z * n_r + me_r

    strides = (n_r, nx * nyl * nc, nyl * nc, nc, 1)
    digits = []
    for at, n, stride in zip((z, yh, x, yl, c), dims, strides):
        digits.append([jnp.where(at + k >= n, at + k - n, at + k) * stride if k else at * stride for k in range(n)])

    def hops(offset):
        dz, a, b, d, e = offset
        return min(dz, nz - dz) + min(b, nx - b) + (2 if a and not d else 1 if a or d else 0)

    def peers(free):
        spans = [range(n) if f else (0,) for n, f in zip(dims, free)]
        offsets = [o for o in itertools.product(*spans) if any(o)]
        return sorted(offsets, key=lambda o: -hops(o))

    def number(offset):
        return sum(digits[i][k] for i, k in enumerate(offset))

    s_peers = peers((0, 1, 1, 0, 0))
    r_peers = peers((0, 1, 1, 1, 1))
    z_peers = peers((1, 0, 0, 0, 0))
    all_peers = peers((1, 1, 1, 1, 1))
    base = digits[0][0]

    def slice_of(offset):
        return (digits[1][offset[1]] + digits[2][offset[2]]) // (nyl * nc)

    def first_tile(q):
        return (q * tiles) // n_s

    def remote(src, dst, ssem, rsem, where):
        return pltpu.make_async_remote_copy(src, dst, ssem, rsem, device_id=where, device_id_type=LOGICAL)

    def wait_recv(ref, sem):
        remote(ref, ref, sem, sem, number(s_peers[0])).wait_recv()

    def wait_send(ref, sem):
        remote(ref, ref, sem, sem, number(s_peers[0])).wait_send()

    my_off = pl.multiple_of(first_tile(me_s) * LANE, LANE)

    def extra(q):
        return first_tile(q + 1) - first_tile(q) > nt

    if_extra = pl.when(extra(me_s))
    last = pl.ds(nt * LANE, LANE)

    own_rows = pl.ds(pl.multiple_of(me_s * 32, 32), 32)

    def local_copies(t0, tn):
        here = pl.ds(pl.multiple_of(my_off + t0 * LANE, LANE), tn * LANE)
        there = pl.ds(t0 * LANE, tn * LANE)
        return [pltpu.make_async_copy(miller_hbm.at[:, here], mil_buf.at[:, there], loc_sem.at[0]),
                pltpu.make_async_copy(proj_hbm.at[:, :, here], p_buf.at[:, beta, :, there], loc_sem.at[1]),
                pltpu.make_async_copy(psi_hbm.at[:, :, here], psi_buf.at[:, own_rows, there], loc_sem.at[2])]

    small = [pltpu.make_async_copy(a, b, loc_sem.at[3 + n]) for n, (a, b) in enumerate((
        (occ_hbm, occ_in), (lat_hbm, lat_ref), (spec_hbm, spec_ref), (cnt_hbm, cnt_ref), (coup_hbm, coup_ref)))]

    bar = pltpu.get_barrier_semaphore()
    for o in sorted(z_peers + r_peers, key=lambda o: -hops(o)):
        pl.semaphore_signal(bar, 1, device_id=number(o), device_id_type=LOGICAL)
    occ_row[...] = jnp.zeros_like(occ_row)
    for cp in small + local_copies(0, nt):
        cp.start()

    @if_extra
    def _():
        for cp in local_copies(nt, 1):
            cp.start()

    pl.semaphore_wait(bar, n_r - 1 + nz - 1)

    def send_slices(src, dst_of, ssem, rsem):
        for i, (t0, tn) in enumerate(chunks):
            for o in s_peers:
                q, where = slice_of(o), number(o)
                off = pl.multiple_of((first_tile(q) + t0) * LANE, LANE)
                remote(src.at[:, :, pl.ds(off, tn * LANE)], dst_of(pl.ds(t0 * LANE, tn * LANE)), ssem.at[i], rsem.at[i], where).start()
                if i == n_chunk - 1:

                    @pl.when(extra(q))
                    def _():
                        end = pl.multiple_of((first_tile(q) + nt) * LANE, LANE)
                        remote(src.at[:, :, pl.ds(end, LANE)], dst_of(last), ssem.at[n_chunk], rsem.at[n_chunk], where).start()

    send_slices(proj_hbm, lambda part: p_buf.at[:, beta, :, part], psend, precv)
    send_slices(psi_hbm, lambda part: psi_buf.at[:, own_rows, part], ssend, srecv)

    small[0].wait()
    occ_row[:, :32] = occ_in[...]
    occ_buf[me_s] = pltpu.roll(occ_row[...], me_s * 32, 1)
    for o in s_peers:
        remote(occ_buf.at[me_s], occ_buf.at[me_s], osend, orecv, number(o)).start()

    kp = w_buf.shape[1]
    used = (nt + 1) * LANE
    mine = local_copies(0, nt)
    more = local_copies(nt, 1)
    mine[0].wait()
    if_extra(lambda: more[0].wait())

    def clear(at, size):
        mil_buf[:, pl.ds(at, size)] = jnp.zeros((3, size), jnp.int32)
        psi_buf[:, :, pl.ds(at, size)] = jnp.zeros((2, psi_buf.shape[1], size), BF16)
        p_buf[:, :, :, pl.ds(at, size)] = jnp.zeros((2, p_buf.shape[1], PROJ, size), BF16)

    if kp > used:
        clear(used, kp - used)

    @pl.when(jnp.logical_not(extra(me_s)))
    def _():
        clear(nt * LANE, LANE)

    small[1].wait()
    idx = [mil_buf[a : a + 1, :].astype(F32) for a in range(3)]
    co = [(idx[0] * lat_ref[0, a] + idx[1] * lat_ref[1, a] + idx[2] * lat_ref[2, a]) / MILLER for a in range(3)]
    iso = (co[0] * co[0] + co[1] * co[1] + co[2] * co[2]) / 3.0
    rows = list(co)
    for a, b in ((0, 0), (1, 1), (2, 2), (0, 1), (0, 2), (1, 2)):
        prod = co[a] * co[b]
        rows.append(prod - iso if a == b else prod)
    for m, row in enumerate(rows):
        w_buf[m : m + 1, :] = row
    facc[...] = jnp.zeros_like(facc)
    sacc[...] = jnp.zeros_like(sacc)
    acc[...] = jnp.zeros_like(acc)

    mine[1].wait()
    if_extra(lambda: more[1].wait())
    plane = pl.ds(pl.multiple_of(z * n_s, n_s), n_s)

    def pass_on(part, i):
        for o in z_peers:
            remote(p_buf.at[:, plane, :, part], p_buf.at[:, plane, :, part], zsend.at[i], zrecv.at[i], number(o)).start()

    for i, (t0, tn) in enumerate(chunks):
        part = pl.ds(t0 * LANE, tn * LANE)
        with jax.named_scope(f'wp{i}'):
            wait_recv(p_buf.at[:, pl.ds(0, n_s - 1), :, part], precv.at[i])
        pass_on(part, i)
        if i == n_chunk - 1:

            @if_extra
            def _():
                wait_recv(p_buf.at[:, pl.ds(0, n_s - 1), :, last], precv.at[n_chunk])
                pass_on(last, n_chunk)

    mine[2].wait()
    if_extra(lambda: more[2].wait())
    nb = psi_buf.shape[1]
    na = p_buf.shape[1]
    for i, (t0, tn) in enumerate(chunks):
        part = pl.ds(t0 * LANE, tn * LANE)
        with jax.named_scope(f'wz{i}'):
            wait_recv(p_buf.at[:, pl.ds(0, n_s * (nz - 1)), :, part], zrecv.at[i])
        with jax.named_scope(f'wpsi{i}'):
            wait_recv(psi_buf.at[:, pl.ds(0, 32 * (n_s - 1)), part], srecv.at[i])
        if i == n_chunk - 1:

            @if_extra
            def _():
                wait_recv(p_buf.at[:, pl.ds(0, n_s * (nz - 1)), :, last], zrecv.at[n_chunk])
                wait_recv(psi_buf.at[:, pl.ds(0, 32 * (n_s - 1)), last], srecv.at[n_chunk])

            tn = tn + 1
            part = pl.ds(t0 * LANE, tn * LANE)
        rhs = psi_buf[:, :, part].reshape(2 * nb, tn * LANE)
        lhs = p_buf[:, :, :, part].reshape(2 * na * PROJ, tn * LANE)
        acc[...] += lax.dot_general(lhs, rhs, (((1,), (1,)), ((), ())), preferred_element_type=F32)

    np_ = na * PROJ
    b_send[:, 0] = (acc[:np_, :nb] + acc[np_:, nb:]).reshape(na, PROJ, nb).astype(BF16)
    b_send[:, 1] = (acc[:np_, nb:] - acc[np_:, :nb]).reshape(na, PROJ, nb).astype(BF16)

    for o in r_peers:
        remote(b_send.at[number(o) - base], rs_buf.at[me_r], rsend, rrecv, number(o)).start()
    rs_buf[me_r] = b_send[me_r]
    for cp in small[2:]:
        cp.wait()
    wait_recv(occ_buf.at[pl.ds(0, n_s - 1)], orecv)
    occ = jnp.sum(occ_buf[...], axis=0)
    kind = spec_ref[me_r]
    count = cnt_ref[me_r]
    mat = coup_ref[kind]
    act = (lax.broadcasted_iota(jnp.int32, (PROJ, PROJ), 0) < count) & (lax.broadcasted_iota(jnp.int32, (PROJ, PROJ), 1) < count)
    mat = jnp.where(act, mat, 0.0)
    wait_recv(rs_buf.at[pl.ds(0, n_r - 1)], rrecv)
    total = jnp.sum(rs_buf[...].astype(F32), axis=0)
    for h in range(2):
        mixed = jnp.zeros((PROJ, nb), F32)
        for i in range(PROJ):
            mixed = mixed + mat[:, i : i + 1] * total[h, i : i + 1, :]
        uv_buf[h, me_r] = (mixed * occ).astype(BF16)

    for o in r_peers:
        remote(uv_buf.at[:, me_r], uv_buf.at[:, me_r], asend, arecv, number(o)).start()
    wait_recv(uv_buf.at[:, pl.ds(0, n_r - 1)], arecv)

    u = uv_buf[0].reshape(np_, nb)
    v = uv_buf[1].reshape(np_, nb)
    negv[0] = u
    negv[1] = v
    negv[2] = -v

    wide = 256

    def block(i, carry):
        cols = pl.ds(pl.multiple_of(i * wide, wide), wide)
        re = psi_buf[0, :, cols]
        im = psi_buf[1, :, cols]
        dot = functools.partial(jnp.dot, preferred_element_type=F32)
        y_re = dot(negv[0], re) + dot(negv[1], im)
        y_im = dot(negv[0], im) + dot(negv[2], re)
        p_re = p_buf[0, :, :, cols].astype(F32).reshape(np_, wide)
        p_im = p_buf[1, :, :, cols].astype(F32).reshape(np_, wide)
        e_im = (p_re * y_im - p_im * y_re).reshape(na, PROJ, wide)
        e_re = jnp.sum((p_re * y_re + p_im * y_im).reshape(na, PROJ, wide), axis=0)
        for a in range(3):
            t = e_im * w_buf[a : a + 1, cols].reshape(1, 1, wide)
            facc[a] += t[:, :, :LANE] + t[:, :, LANE:]
        for m in range(6):
            t = e_re * w_buf[3 + m : 4 + m, cols]
            sacc[m] += t[:, :LANE] + t[:, LANE:]
        return carry

    lax.fori_loop(0, kp // wide, block, 0)

    lane = lax.broadcasted_iota(jnp.int32, (1, LANE), 1)
    row = jnp.zeros((1, LANE), F32)
    for a in range(3):
        f = jnp.sum(facc[a], axis=1)
        f = jnp.concatenate([jnp.zeros((a * na, LANE), F32), f, jnp.zeros((LANE - (a + 1) * na, LANE), F32)][0 if a else 1 :], axis=0)
        row = row + jnp.sum(f.T, axis=0, keepdims=True)
    for m in range(6):
        row = row + jnp.where(lane == 3 * na + m, jnp.sum(sacc[m], keepdims=True), 0.0)
    tot[me] = row
    for o in all_peers:
        remote(tot.at[me], tot.at[me], fsend, frecv, number(o)).start()
    wait_recv(tot.at[pl.ds(0, n_all - 1)], frecv)
    res = jnp.sum(tot[...], axis=0)
    out_ref[...] = res

    for i, (t0, tn) in enumerate(chunks):
        part = pl.ds(t0 * LANE, tn * LANE)
        wait_send(p_buf.at[:, pl.ds(0, n_s - 1), :, part], psend.at[i])
        wait_send(psi_buf.at[:, pl.ds(0, 32 * (n_s - 1)), part], ssend.at[i])
        wait_send(p_buf.at[:, pl.ds(0, n_s * (nz - 1)), :, part], zsend.at[i])
    for o in s_peers:

        @pl.when(extra(slice_of(o)))
        def _():
            wait_send(p_buf.at[:, 0, :, last], psend.at[n_chunk])
            wait_send(psi_buf.at[:, pl.ds(0, 32), last], ssend.at[n_chunk])

    if_extra(lambda: wait_send(p_buf.at[:, pl.ds(0, n_s * (nz - 1)), :, last], zsend.at[n_chunk]))
    wait_send(occ_buf.at[pl.ds(0, n_s - 1)], osend)
    wait_send(rs_buf.at[pl.ds(0, n_r - 1)], rsend)
    wait_send(uv_buf.at[:, pl.ds(0, n_r - 1)], asend)
    wait_send(tot.at[pl.ds(0, n_all - 1)], fsend)


def finish(dims, na, scales, row_ref, force_ref, stress_ref):
    res = row_ref[...]
    beta = (lax.axis_index("z") * dims[1] + lax.axis_index("yh")) * dims[2] + lax.axis_index("x")
    lane = lax.broadcasted_iota(jnp.int32, (1, LANE), 1)
    own = [jnp.sum(jnp.where(lane == a * na + beta, res, 0.0), axis=1, keepdims=True) for a in range(3)]
    force_ref[...] = jnp.where(lane[:, :3] == 0, own[0], jnp.where(lane[:, :3] == 1, own[1], own[2])) * scales[0]
    i0 = lax.broadcasted_iota(jnp.int32, (3, 3), 0)
    i1 = lax.broadcasted_iota(jnp.int32, (3, 3), 1)
    st = jnp.zeros((3, 3), F32)
    for m, (a, b) in enumerate(((0, 0), (1, 1), (2, 2), (0, 1), (0, 2), (1, 2))):
        val = jnp.sum(jnp.where(lane == 3 * na + m, res, 0.0), axis=1, keepdims=True)
        hit = ((i0 == a) & (i1 == b)) | ((i0 == b) & (i1 == a))
        st = st + jnp.where(hit, val, 0.0)
    stress_ref[...] = st * scales[1]


def body(dims, psi, proj, miller, lattice, occupation, species, proj_count, coupling):
    nz, nyh, nx, nyl, nc = dims
    n_s = nyh * nx
    n_r = n_s * nyl * nc
    bands = psi.shape[1]
    tiles = psi.shape[2] // LANE
    atoms = species.shape[0]
    nt = tiles // n_s
    sizes = []
    left = nt
    for want in (6, 5, 4):
        if left > want:
            sizes.append(want)
            left -= want
    sizes.append(left)
    chunks, at = [], 0
    for n in sizes:
        chunks.append((at, n))
        at += n
    kp = -(-(nt + 1) * LANE // 256) * 256
    nb = n_s * bands
    band_total = nb * nz
    scales = (2.0 / (PROJ * math.sqrt(band_total)), 1.0 / (PROJ * math.sqrt(atoms * band_total)))
    any_spec = pl.BlockSpec(memory_space=pl.ANY)
    vmem = pl.BlockSpec(memory_space=pltpu.VMEM)
    dma = pltpu.SemaphoreType.DMA
    nch = len(chunks)
    row = pl.pallas_call(
        functools.partial(kernel, dims, nt, tiles, tuple(chunks)),
        out_shape=jax.ShapeDtypeStruct((1, LANE), F32),
        in_specs=[any_spec] * 8,
        out_specs=vmem,
        scratch_shapes=[
            pltpu.VMEM((2, nb, kp), BF16),
            pltpu.VMEM((2, atoms, PROJ, kp), BF16),
            pltpu.VMEM((3, kp), jnp.int32),
            pltpu.VMEM((n_s, 1, nb), F32),
            pltpu.VMEM((16, kp), F32),
            pltpu.VMEM((2 * atoms * PROJ, 2 * nb), F32),
            pltpu.VMEM((atoms, 2, PROJ, nb), BF16),
            pltpu.VMEM((n_r, 2, PROJ, nb), BF16),
            pltpu.VMEM((2, n_r, PROJ, nb), BF16),
            pltpu.VMEM((3, atoms * PROJ, nb), BF16),
            pltpu.VMEM((3, atoms, PROJ, LANE), F32),
            pltpu.VMEM((6, PROJ, LANE), F32),
            pltpu.VMEM((nz * n_r, 1, LANE), F32),
            pltpu.SMEM((3, 3), F32), pltpu.SMEM(species.shape, jnp.int32), pltpu.SMEM(species.shape, jnp.int32),
            pltpu.VMEM(coupling.shape, F32), pltpu.VMEM((1, nb), F32), pltpu.VMEM((1, bands), F32),
            dma((8,)), *[dma((nch + 1,))] * 6, dma, dma, dma, dma, dma, dma, dma, dma,
        ],
        compiler_params=pltpu.CompilerParams(collective_id=0, has_side_effects=True, vmem_limit_bytes=58 << 20),
        name="plane_kernel",
    )(psi, proj, miller, lattice, occupation[None], species, proj_count, coupling)
    force, stress = pl.pallas_call(
        functools.partial(finish, dims, atoms, scales),
        out_shape=(jax.ShapeDtypeStruct((1, 3), F32), jax.ShapeDtypeStruct((3, 3), F32)),
        in_specs=[vmem],
        out_specs=(vmem, vmem),
        name="finish",
    )(row)
    return force.T, stress


def solution(mesh, dims=(4, 2, 4, 2, 2)):
    finer = Mesh(mesh.devices.reshape(dims), AXES)
    band, gvec = ("z", "yh", "x"), ("yl", "core")
    in_specs = (P(None, band, gvec), P(None, band, gvec), P(None, gvec), P(), P(band), P(), P(), P())
    return jax.shard_map(functools.partial(body, dims), mesh=finer, in_specs=in_specs, out_specs=(P(None, band), P()), check_vma=False)
```

```python
import functools
import itertools
import math

import jax
import jax.numpy as jnp
from jax import lax
from jax.experimental import pallas as pl
from jax.experimental.pallas import tpu as pltpu
from jax.sharding import Mesh
from jax.sharding import PartitionSpec as P

PROJ = 8
MILLER = 24.0
LANE = 128
HALF = 64
LOGICAL = pl.DeviceIdType.LOGICAL
F32 = jnp.float32
BF16 = jnp.bfloat16
AXES = ("z", "yh", "x", "yl", "core")
STRESS = ((0, 0), (1, 1), (2, 2), (0, 1), (0, 2), (1, 2))


def kernel(
    dims, nt, tiles, p_chunks, phases,
    psi_hbm, proj_hbm, miller_hbm, lat_hbm, occ_hbm, spec_hbm, cnt_hbm, coup_hbm,
    out_ref,
    psi_buf, p_buf, mil_buf, occ_buf, w_buf, lat_ref, spec_ref, cnt_ref, coup_ref, occ_row, occ_in, y_buf, facc, sacc, tot,
    *rest,
):
    n_ph = len(phases)
    per = [rest[i * 5 : i * 5 + 5] for i in range(n_ph)]
    loc_sem, psend, precv, zsend, zrecv, osend, orecv, ssend, srecv, rsend, rrecv, asend, arecv, fsend, frecv = rest[5 * n_ph :]
    nz, nyh, nx, nyl, nc = dims
    n_s = nyh * nx
    n_r = n_s * nyl * nc
    n_all = nz * n_r
    z, yh, x, yl, c = (lax.axis_index(a) for a in AXES)
    me_s = yh * nx + x
    me_r = me_s * (nyl * nc) + yl * nc + c
    me = z * n_r + me_r
    beta = z * n_s + me_s
    na = p_buf.shape[1]
    np_ = na * PROJ
    kp = w_buf.shape[1]

    strides = (n_r, nx * nyl * nc, nyl * nc, nc, 1)
    digits = []
    for at, n, stride in zip((z, yh, x, yl, c), dims, strides):
        digits.append([jnp.where(at + k >= n, at + k - n, at + k) * stride if k else at * stride for k in range(n)])

    def hops(offset):
        dz, a, b, d, e = offset
        return min(dz, nz - dz) + min(b, nx - b) + (2 if a and not d else 1 if a or d else 0)

    def peers(free):
        spans = [range(n) if f else (0,) for n, f in zip(dims, free)]
        offsets = [o for o in itertools.product(*spans) if any(o)]
        return sorted(offsets, key=lambda o: -hops(o))

    def number(offset):
        return sum(digits[i][k] for i, k in enumerate(offset))

    s_peers = peers((0, 1, 1, 0, 0))
    r_peers = peers((0, 1, 1, 1, 1))
    z_peers = peers((1, 0, 0, 0, 0))
    all_peers = peers((1, 1, 1, 1, 1))
    base = digits[0][0]

    def slice_of(offset):
        return (digits[1][offset[1]] + digits[2][offset[2]]) // (nyl * nc)

    def first_tile(q):
        return (q * tiles) // n_s

    def extra(q):
        return first_tile(q + 1) - first_tile(q) > nt

    def remote(src, dst, ssem, rsem, where):
        return pltpu.make_async_remote_copy(src, dst, ssem, rsem, device_id=where, device_id_type=LOGICAL)

    def wait_recv(ref, sem):
        remote(ref, ref, sem, sem, number(s_peers[0])).wait_recv()

    def wait_send(ref, sem):
        remote(ref, ref, sem, sem, number(s_peers[0])).wait_send()

    my_off = pl.multiple_of(first_tile(me_s) * LANE, LANE)
    if_extra = pl.when(extra(me_s))
    last = pl.ds(nt * LANE, LANE)

    def cols(chunk):
        return pl.ds(chunk[0] * LANE, chunk[1] * LANE)

    def local_copies(t0, tn):
        here = pl.ds(pl.multiple_of(my_off + t0 * LANE, LANE), tn * LANE)
        there = pl.ds(t0 * LANE, tn * LANE)
        return [pltpu.make_async_copy(miller_hbm.at[:, here], mil_buf.at[:, there], loc_sem.at[0]),
                pltpu.make_async_copy(proj_hbm.at[:, :, here], p_buf.at[:, beta, :, there], loc_sem.at[1]),
                pltpu.make_async_copy(psi_hbm.at[:, :, :, here], psi_buf.at[:, :, me_s, :, there], loc_sem.at[2])]

    small = [pltpu.make_async_copy(a, b, loc_sem.at[3 + n]) for n, (a, b) in enumerate((
        (occ_hbm, occ_in), (lat_hbm, lat_ref), (spec_hbm, spec_ref), (cnt_hbm, cnt_ref), (coup_hbm, coup_ref)))]

    bar = pltpu.get_barrier_semaphore()
    for o in sorted(z_peers + r_peers, key=lambda o: -hops(o)):
        pl.semaphore_signal(bar, 1, device_id=number(o), device_id_type=LOGICAL)
    occ_row[...] = jnp.zeros_like(occ_row)
    for cp in small + local_copies(0, nt):
        cp.start()

    @if_extra
    def _():
        for cp in local_copies(nt, 1):
            cp.start()

    pl.semaphore_wait(bar, n_r - 1 + nz - 1)

    def send_slices(src, dst_of, chunks, ssem, rsem):
        for i, (t0, tn) in enumerate(chunks):
            for o in s_peers:
                q, where = slice_of(o), number(o)
                off = pl.multiple_of((first_tile(q) + t0) * LANE, LANE)
                remote(src(pl.ds(off, tn * LANE)), dst_of(cols((t0, tn))), ssem(i), rsem(i), where).start()
                if i == 0:

                    @pl.when(extra(q))
                    def _():
                        end = pl.multiple_of((first_tile(q) + nt) * LANE, LANE)
                        remote(src(pl.ds(end, LANE)), dst_of(last), ssem(len(chunks)), rsem(len(chunks)), where).start()

    send_slices(lambda part: proj_hbm.at[:, :, part], lambda part: p_buf.at[:, beta, :, part], p_chunks, lambda i: psend.at[i], lambda i: precv.at[i])
    for h, (g0, gn, chunks) in enumerate(phases):
        send_slices(lambda part: psi_hbm.at[:, pl.ds(g0, gn), :, part], lambda part: psi_buf.at[:, pl.ds(g0, gn), me_s, :, part],
                    chunks, lambda i: ssend.at[h, i], lambda i: srecv.at[h, i])

    lane = lax.broadcasted_iota(jnp.int32, (1, LANE), 1)
    small[0].wait()
    n_g = occ_buf.shape[1]
    occ_row[:, : occ_in.shape[1]] = occ_in[...]
    raw = occ_row[...]
    mine8 = (lane >= me_s * 8) & (lane < me_s * 8 + 8)
    for g in range(n_g):
        occ_buf[me_s, g : g + 1, :] = jnp.where(mine8, pltpu.roll(raw, me_s * 8 + (LANE - 8 * g) % LANE, 1), 0.0)
    for o in s_peers:
        remote(occ_buf.at[me_s], occ_buf.at[me_s], osend, orecv, number(o)).start()

    mine = local_copies(0, nt)
    more = local_copies(nt, 1)
    mine[0].wait()
    if_extra(lambda: more[0].wait())

    def clear(at, size):
        mil_buf[:, pl.ds(at, size)] = jnp.zeros((3, size), jnp.int32)
        psi_buf[:, :, :, :, pl.ds(at, size)] = jnp.zeros((*psi_buf.shape[:4], size), BF16)
        p_buf[:, :, :, pl.ds(at, size)] = jnp.zeros((2, na, PROJ, size), BF16)

    clear((nt + 1) * LANE, kp - (nt + 1) * LANE)

    @pl.when(jnp.logical_not(extra(me_s)))
    def _():
        clear(nt * LANE, LANE)

    small[1].wait()
    idx = [mil_buf[a : a + 1, :].astype(F32) for a in range(3)]
    co = [(idx[0] * lat_ref[0, a] + idx[1] * lat_ref[1, a] + idx[2] * lat_ref[2, a]) / MILLER for a in range(3)]
    iso = (co[0] * co[0] + co[1] * co[1] + co[2] * co[2]) / 3.0
    rows = list(co)
    for a, b in STRESS:
        prod = co[a] * co[b]
        rows.append(prod - iso if a == b else prod)
    for m, row in enumerate(rows):
        w_buf[m : m + 1, :] = row
    facc[...] = jnp.zeros_like(facc)
    sacc[...] = jnp.zeros_like(sacc)

    mine[1].wait()
    if_extra(lambda: more[1].wait())
    n_pc = len(p_chunks)
    up, down = number((1, 0, 0, 0, 0)), number((nz - 1, 0, 0, 0, 0))

    def plane(k):
        return pl.ds(pl.multiple_of(digits[0][k % nz] // n_r * n_s, n_s), n_s)

    def z_own(part, i):
        wait_recv(p_buf.at[:, pl.ds(0, n_s - 1), :, part], precv.at[i])
        ref = p_buf.at[:, plane(0), :, part]
        remote(ref, ref, zsend.at[0, i], zrecv.at[0, i], up).start()
        remote(ref, ref, zsend.at[1, i], zrecv.at[1, i], down).start()

    def z_next(part, i):
        wait_recv(p_buf.at[:, plane(0), :, part], zrecv.at[0, i])
        ref = p_buf.at[0, plane(-1), :, part]
        remote(ref, ref, zsend.at[2, i], zrecv.at[2, i], up).start()
        wait_recv(p_buf.at[:, plane(0), :, part], zrecv.at[1, i])
        ref = p_buf.at[1, plane(1), :, part]
        remote(ref, ref, zsend.at[3, i], zrecv.at[3, i], down).start()

    def z_end(part, i):
        wait_recv(p_buf.at[0, plane(0), :, part], zrecv.at[2, i])
        wait_recv(p_buf.at[1, plane(0), :, part], zrecv.at[3, i])

    def each_chunk(step):
        for i, chunk in enumerate(p_chunks):
            step(cols(chunk), i)
            if i == 0:
                if_extra(lambda: step(last, n_pc))

    each_chunk(z_own)
    each_chunk(z_next)

    mine[2].wait()
    if_extra(lambda: more[2].wait())
    for cp in small[2:]:
        cp.wait()
    kind = spec_ref[me_r]
    count = cnt_ref[me_r]
    act = (lax.broadcasted_iota(jnp.int32, (PROJ, PROJ), 0) < count) & (lax.broadcasted_iota(jnp.int32, (PROJ, PROJ), 1) < count)
    mat = jnp.where(act, coup_ref[kind], 0.0)
    front = lane < HALF
    z_done = [-1]

    def z_arrived(upto):
        while z_done[0] < n_pc - 1 and (z_done[0] < 0 or sum(p_chunks[z_done[0]]) < upto):
            z_done[0] += 1
            i = z_done[0]
            with jax.named_scope(f"wz{i}"):
                z_end(cols(p_chunks[i]), i)
            if i == 0:
                if_extra(lambda: z_end(last, n_pc))

    def gather_chunk(h, i):
        g0, gn, chunks = phases[h]
        acc = per[h][0]
        z_arrived(sum(chunks[i]))
        with jax.named_scope(f"wpsi{h}{i}"):
            wait_recv(psi_buf.at[:, pl.ds(g0, gn), pl.ds(0, n_s - 1), :, cols(chunks[i])], srecv.at[h, i])
        parts = [cols(chunks[i])]
        if i == 0:
            if_extra(lambda: wait_recv(psi_buf.at[:, pl.ds(g0, gn), pl.ds(0, n_s - 1), :, last], srecv.at[h, len(chunks)]))
            parts.append(pl.ds(nt * LANE, kp - nt * LANE))
        total = None if i == 0 else acc[...]
        for part in parts:
            rhs = jnp.concatenate([psi_buf[r, g, :, :, part].reshape(HALF, part.size) for g in range(g0, g0 + gn) for r in range(2)], axis=0)
            lhs = p_buf[:, :, :, part].reshape(2 * np_, part.size)
            term = lax.dot_general(lhs, rhs, (((1,), (1,)), ((), ())), preferred_element_type=F32)
            total = term if total is None else total + term
        acc[...] = total

    def reduce_start(h):
        acc, b_send, rs_buf = per[h][:3]
        for g in range(phases[h][1]):
            tile = pl.ds(g * LANE, LANE)
            low = pltpu.roll(acc[np_:, tile], HALF, 1)
            b_send[:, :, tile] = (acc[:np_, tile] + jnp.where(front, low, -low)).reshape(na, PROJ, LANE).astype(BF16)
        for o in r_peers:
            remote(b_send.at[number(o) - base], rs_buf.at[me_r], rsend.at[h], rrecv.at[h], number(o)).start()
        rs_buf[me_r] = b_send[me_r]

    def mix_and_spread(h):
        rs_buf, uv_buf = per[h][2:4]
        if h == 0:
            wait_recv(occ_buf.at[pl.ds(0, n_s - 1)], orecv)
        with jax.named_scope(f"rs_wait{h}"):
            wait_recv(rs_buf.at[pl.ds(0, n_r - 1)], rrecv.at[h])
        total = jnp.sum(rs_buf[...].astype(F32), axis=0)
        mixed = jnp.zeros_like(total)
        for i in range(PROJ):
            mixed = mixed + mat[:, i : i + 1] * total[i : i + 1, :]
        occ = jnp.sum(occ_buf[...], axis=0)
        occ = occ + pltpu.roll(occ, HALF, 1)
        for g in range(phases[h][1]):
            tile = pl.ds(g * LANE, LANE)
            at = phases[h][0] + g
            uv_buf[me_r, :, tile] = (mixed[:, g * LANE : (g + 1) * LANE] * occ[at : at + 1, :]).astype(BF16)
        for o in r_peers:
            remote(uv_buf.at[me_r], uv_buf.at[me_r], asend.at[h], arecv.at[h], number(o)).start()

    def collect(h):
        uv_buf, left = per[h][3:5]
        with jax.named_scope(f"ag_wait{h}"):
            wait_recv(uv_buf.at[pl.ds(0, n_r - 1)], arecv.at[h])
        uv = uv_buf[...].reshape(np_, phases[h][1] * LANE)
        left[:np_] = uv
        for g in range(phases[h][1]):
            tile = pl.ds(g * LANE, LANE)
            turned = pltpu.roll(uv[:, g * LANE : (g + 1) * LANE].astype(F32), HALF, 1)
            left[np_:, tile] = jnp.where(front, -turned, turned).astype(BF16)

    wide = 256

    def weighted(h, i):
        g0, gn, _ = phases[h]
        part = pl.ds(pl.multiple_of(i * wide, wide), wide)
        rhs = jnp.concatenate([psi_buf[r, g, :, :, part].reshape(HALF, wide) for g in range(g0, g0 + gn) for r in range(2)], axis=0)
        return part, jnp.dot(per[h][4][...], rhs, preferred_element_type=F32)

    def early_block(h, i, carry):
        part, y = weighted(h, i)
        y_buf[:, part] = y if h == 0 else y_buf[:, part] + y
        return carry

    def block(i, carry):
        part, y = weighted(n_ph - 1, i)
        if n_ph > 1:
            y = y + y_buf[:, part]
        y_re, y_im = y[:np_], y[np_:]
        p_re = p_buf[0, :, :, part].astype(F32).reshape(np_, wide)
        p_im = p_buf[1, :, :, part].astype(F32).reshape(np_, wide)
        e_im = (p_re * y_im - p_im * y_re).reshape(na, PROJ, wide)
        e_re = jnp.sum((p_re * y_re + p_im * y_im).reshape(na, PROJ, wide), axis=0)
        for a in range(3):
            t = e_im * w_buf[a : a + 1, part].reshape(1, 1, wide)
            facc[a] += t[:, :, :LANE] + t[:, :, LANE:]
        for m in range(6):
            t = e_re * w_buf[3 + m : 4 + m, part]
            sacc[m] += t[:, :LANE] + t[:, LANE:]
        return carry

    for i in range(len(phases[0][2])):
        gather_chunk(0, i)
    reduce_start(0)
    if n_ph > 1:
        for i in range(len(phases[1][2])):
            gather_chunk(1, i)
        reduce_start(1)
        mix_and_spread(0)
    mix_and_spread(n_ph - 1)
    if n_ph > 1:
        collect(0)
        lax.fori_loop(0, kp // wide, functools.partial(early_block, 0), 0, unroll=UNROLL)
    collect(n_ph - 1)
    lax.fori_loop(0, kp // wide, block, 0, unroll=UNROLL)

    row = jnp.zeros((1, LANE), F32)
    for a in range(3):
        f = jnp.sum(facc[a], axis=1)
        f = jnp.concatenate([jnp.zeros((a * na, LANE), F32), f, jnp.zeros((LANE - (a + 1) * na, LANE), F32)][0 if a else 1 :], axis=0)
        row = row + jnp.sum(f.T, axis=0, keepdims=True)
    for m in range(6):
        row = row + jnp.where(lane == 3 * na + m, jnp.sum(sacc[m], keepdims=True), 0.0)
    tot[me] = row
    for o in all_peers:
        remote(tot.at[me], tot.at[me], fsend, frecv, number(o)).start()
    wait_recv(tot.at[pl.ds(0, n_all - 1)], frecv)
    out_ref[...] = jnp.sum(tot[...], axis=0)

    for i, chunk in enumerate(p_chunks):
        wait_send(p_buf.at[:, pl.ds(0, n_s - 1), :, cols(chunk)], psend.at[i])

    def z_sent(part, i):
        for k in range(4):
            wait_send(p_buf.at[:, plane(0), :, part] if k < 2 else p_buf.at[0, plane(0), :, part], zsend.at[k, i])

    each_chunk(z_sent)
    for h, (g0, gn, chunks) in enumerate(phases):
        for i, chunk in enumerate(chunks):
            wait_send(psi_buf.at[:, pl.ds(g0, gn), pl.ds(0, n_s - 1), :, cols(chunk)], ssend.at[h, i])
        wait_send(per[h][2].at[pl.ds(0, n_r - 1)], rsend.at[h])
        wait_send(per[h][3].at[pl.ds(0, n_r - 1)], asend.at[h])
    for o in s_peers:

        @pl.when(extra(slice_of(o)))
        def _():
            wait_send(p_buf.at[:, 0, :, last], psend.at[n_pc])
            for h, (g0, gn, chunks) in enumerate(phases):
                wait_send(psi_buf.at[:, pl.ds(g0, gn), 0, :, last], ssend.at[h, len(chunks)])

    wait_send(occ_buf.at[pl.ds(0, n_s - 1)], osend)
    wait_send(tot.at[pl.ds(0, n_all - 1)], fsend)


def finish(dims, na, scales, row_ref, force_ref, stress_ref):
    res = row_ref[...]
    beta = (lax.axis_index("z") * dims[1] + lax.axis_index("yh")) * dims[2] + lax.axis_index("x")
    lane = lax.broadcasted_iota(jnp.int32, (1, LANE), 1)
    own = [jnp.sum(jnp.where(lane == a * na + beta, res, 0.0), axis=1, keepdims=True) for a in range(3)]
    force_ref[...] = jnp.where(lane[:, :3] == 0, own[0], jnp.where(lane[:, :3] == 1, own[1], own[2])) * scales[0]
    i0 = lax.broadcasted_iota(jnp.int32, (3, 3), 0)
    i1 = lax.broadcasted_iota(jnp.int32, (3, 3), 1)
    st = jnp.zeros((3, 3), F32)
    for m, (a, b) in enumerate(STRESS):
        val = jnp.sum(jnp.where(lane == 3 * na + m, res, 0.0), axis=1, keepdims=True)
        hit = ((i0 == a) & (i1 == b)) | ((i0 == b) & (i1 == a))
        st = st + jnp.where(hit, val, 0.0)
    stress_ref[...] = st * scales[1]


def cut(total, wants):
    chunks, at = [], 0
    for n in wants:
        if at + n < total:
            chunks.append((at, n))
            at += n
    chunks.append((at, total - at))
    return tuple(chunks)


UNROLL = 5
P_CUT = (4, 6)
SETS = ((2, (10,)), (2, (8, 6)))


def body(dims, psi, proj, miller, lattice, occupation, species, proj_count, coupling):
    nz, nyh, nx, nyl, nc = dims
    n_s = nyh * nx
    n_r = n_s * nyl * nc
    bands = psi.shape[1]
    n_g = bands // 8
    tiles = psi.shape[2] // LANE
    atoms = species.shape[0]
    nt = tiles // n_s
    p_chunks = cut(nt, P_CUT)
    phases, at = [], 0
    for gn, wants in SETS:
        phases.append((at, gn, cut(nt, wants)))
        at += gn
    n_ph = len(phases)
    most = max(len(chunks) for _, _, chunks in phases) + 1
    n_pc = len(p_chunks) + 1
    kp = -(-(nt + 1) * LANE // 256) * 256
    band_total = bands * n_s * nz
    scales = (2.0 / (PROJ * math.sqrt(band_total)), 1.0 / (PROJ * math.sqrt(atoms * band_total)))
    any_spec = pl.BlockSpec(memory_space=pl.ANY)
    vmem = pl.BlockSpec(memory_space=pltpu.VMEM)
    dma = pltpu.SemaphoreType.DMA
    scratch = [
        pltpu.VMEM((2, n_g, n_s, 8, kp), BF16),
        pltpu.VMEM((2, atoms, PROJ, kp), BF16),
        pltpu.VMEM((3, kp), jnp.int32),
        pltpu.VMEM((n_s, n_g, LANE), F32),
        pltpu.VMEM((16, kp), F32),
        pltpu.SMEM((3, 3), F32), pltpu.SMEM(species.shape, jnp.int32), pltpu.SMEM(species.shape, jnp.int32),
        pltpu.VMEM(coupling.shape, F32), pltpu.VMEM((1, LANE), F32), pltpu.VMEM((1, bands), F32),
        pltpu.VMEM((2 * atoms * PROJ, kp), F32),
        pltpu.VMEM((3, atoms, PROJ, LANE), F32),
        pltpu.VMEM((6, PROJ, LANE), F32),
        pltpu.VMEM((nz * n_r, 1, LANE), F32),
    ]
    for _, gn, _ in phases:
        width = gn * LANE
        scratch += [
            pltpu.VMEM((2 * atoms * PROJ, width), F32),
            pltpu.VMEM((atoms, PROJ, width), BF16),
            pltpu.VMEM((n_r, PROJ, width), BF16),
            pltpu.VMEM((n_r, PROJ, width), BF16),
            pltpu.VMEM((2 * atoms * PROJ, width), BF16),
            ]
    scratch += [dma((8,)), *[dma((n_pc,))] * 2, *[dma((4, n_pc))] * 2, dma, dma, *[dma((n_ph, most))] * 2, *[dma((n_ph,))] * 4, dma, dma]
    row = pl.pallas_call(
        functools.partial(kernel, dims, nt, tiles, p_chunks, tuple(phases)),
        out_shape=jax.ShapeDtypeStruct((1, LANE), F32),
        in_specs=[any_spec] * 8,
        out_specs=vmem,
        scratch_shapes=scratch,
        compiler_params=pltpu.CompilerParams(collective_id=0, has_side_effects=True, vmem_limit_bytes=58 << 20),
        name="plane_kernel",
    )(psi.reshape(2, n_g, 8, psi.shape[2]), proj, miller, lattice, occupation[None], species, proj_count, coupling)
    force, stress = pl.pallas_call(
        functools.partial(finish, dims, atoms, scales),
        out_shape=(jax.ShapeDtypeStruct((1, 3), F32), jax.ShapeDtypeStruct((3, 3), F32)),
        in_specs=[vmem],
        out_specs=(vmem, vmem),
        name="finish",
    )(row)
    return force.T, stress


def solution(mesh, dims=(4, 2, 4, 2, 2)):
    finer = Mesh(mesh.devices.reshape(dims), AXES)
    band, gvec = ("z", "yh", "x"), ("yl", "core")
    in_specs = (P(None, band, gvec), P(None, band, gvec), P(None, gvec), P(), P(band), P(), P(), P())
    return jax.shard_map(functools.partial(body, dims), mesh=finer, in_specs=in_specs, out_specs=(P(None, band), P()), check_vma=False)
```

```python
import functools
import itertools
import math

import jax
import jax.numpy as jnp
from jax import lax
from jax.experimental import pallas as pl
from jax.experimental.pallas import tpu as pltpu
from jax.sharding import Mesh
from jax.sharding import PartitionSpec as P

PROJ = 8
MILLER = 24.0
LANE = 128
HALF = 64
LOGICAL = pl.DeviceIdType.LOGICAL
F32 = jnp.float32
BF16 = jnp.bfloat16
AXES = ("z", "yh", "x", "yl", "core")
STRESS = ((0, 0), (1, 1), (2, 2), (0, 1), (0, 2), (1, 2))


def kernel(
    dims, nt, tiles, p_chunks, phases,
    psi_hbm, proj_hbm, miller_hbm, lat_hbm, occ_hbm, spec_hbm, cnt_hbm, coup_hbm,
    out_ref,
    psi_buf, p_buf, mil_buf, occ_buf, w_buf, lat_ref, spec_ref, cnt_ref, coup_ref, occ_row, occ_in, p_wide, facc, sacc, tot,
    *rest,
):
    n_ph = len(phases)
    per = [rest[i * 5 : i * 5 + 5] for i in range(n_ph)]
    loc_sem, psend, precv, zsend, zrecv, osend, orecv, ssend, srecv, rsend, rrecv, asend, arecv, fsend, frecv = rest[5 * n_ph :]
    nz, nyh, nx, nyl, nc = dims
    n_s = nyh * nx
    n_r = n_s * nyl * nc
    n_all = nz * n_r
    z, yh, x, yl, c = (lax.axis_index(a) for a in AXES)
    me_s = yh * nx + x
    me_r = me_s * (nyl * nc) + yl * nc + c
    me = z * n_r + me_r
    beta = z * n_s + me_s
    na = p_buf.shape[1]
    np_ = na * PROJ
    kp = w_buf.shape[1]

    strides = (n_r, nx * nyl * nc, nyl * nc, nc, 1)
    digits = []
    for at, n, stride in zip((z, yh, x, yl, c), dims, strides):
        digits.append([jnp.where(at + k >= n, at + k - n, at + k) * stride if k else at * stride for k in range(n)])

    def hops(offset):
        dz, a, b, d, e = offset
        return min(dz, nz - dz) + min(b, nx - b) + (2 if a and not d else 1 if a or d else 0)

    def peers(free):
        spans = [range(n) if f else (0,) for n, f in zip(dims, free)]
        offsets = [o for o in itertools.product(*spans) if any(o)]
        return sorted(offsets, key=lambda o: -hops(o))

    def number(offset):
        return sum(digits[i][k] for i, k in enumerate(offset))

    s_peers = peers((0, 1, 1, 0, 0))
    r_peers = peers((0, 1, 1, 1, 1))
    z_peers = peers((1, 0, 0, 0, 0))
    all_peers = peers((1, 1, 1, 1, 1))
    base = digits[0][0]

    def slice_of(offset):
        return (digits[1][offset[1]] + digits[2][offset[2]]) // (nyl * nc)

    def first_tile(q):
        return (q * tiles) // n_s

    def extra(q):
        return first_tile(q + 1) - first_tile(q) > nt

    def remote(src, dst, ssem, rsem, where):
        return pltpu.make_async_remote_copy(src, dst, ssem, rsem, device_id=where, device_id_type=LOGICAL)

    def wait_recv(ref, sem):
        remote(ref, ref, sem, sem, number(s_peers[0])).wait_recv()

    def wait_send(ref, sem):
        remote(ref, ref, sem, sem, number(s_peers[0])).wait_send()

    my_off = pl.multiple_of(first_tile(me_s) * LANE, LANE)
    if_extra = pl.when(extra(me_s))
    last = pl.ds(nt * LANE, LANE)

    def cols(chunk):
        return pl.ds(chunk[0] * LANE, chunk[1] * LANE)

    def local_copies(t0, tn):
        here = pl.ds(pl.multiple_of(my_off + t0 * LANE, LANE), tn * LANE)
        there = pl.ds(t0 * LANE, tn * LANE)
        return [pltpu.make_async_copy(miller_hbm.at[:, here], mil_buf.at[:, there], loc_sem.at[0]),
                pltpu.make_async_copy(proj_hbm.at[:, :, here], p_buf.at[:, beta, :, there], loc_sem.at[1]),
                pltpu.make_async_copy(psi_hbm.at[:, :, :, here], psi_buf.at[:, :, me_s, :, there], loc_sem.at[2])]

    small = [pltpu.make_async_copy(a, b, loc_sem.at[3 + n]) for n, (a, b) in enumerate((
        (occ_hbm, occ_in), (lat_hbm, lat_ref), (spec_hbm, spec_ref), (cnt_hbm, cnt_ref), (coup_hbm, coup_ref)))]

    bar = pltpu.get_barrier_semaphore()
    for o in sorted(z_peers + r_peers, key=lambda o: -hops(o)):
        pl.semaphore_signal(bar, 1, device_id=number(o), device_id_type=LOGICAL)
    occ_row[...] = jnp.zeros_like(occ_row)
    for cp in small + local_copies(0, nt):
        cp.start()

    @if_extra
    def _():
        for cp in local_copies(nt, 1):
            cp.start()

    pl.semaphore_wait(bar, n_r - 1 + nz - 1)

    def send_slices(src, dst_of, chunks, ssem, rsem):
        for i, (t0, tn) in enumerate(chunks):
            for o in s_peers:
                q, where = slice_of(o), number(o)
                off = pl.multiple_of((first_tile(q) + t0) * LANE, LANE)
                remote(src(pl.ds(off, tn * LANE)), dst_of(cols((t0, tn))), ssem(i), rsem(i), where).start()
                if i == 0:

                    @pl.when(extra(q))
                    def _():
                        end = pl.multiple_of((first_tile(q) + nt) * LANE, LANE)
                        remote(src(pl.ds(end, LANE)), dst_of(last), ssem(len(chunks)), rsem(len(chunks)), where).start()

    send_slices(lambda part: proj_hbm.at[:, :, part], lambda part: p_buf.at[:, beta, :, part], p_chunks, lambda i: psend.at[i], lambda i: precv.at[i])
    for h, (g0, gn, chunks) in enumerate(phases):
        send_slices(lambda part: psi_hbm.at[:, pl.ds(g0, gn), :, part], lambda part: psi_buf.at[:, pl.ds(g0, gn), me_s, :, part],
                    chunks, lambda i: ssend.at[h, i], lambda i: srecv.at[h, i])

    lane = lax.broadcasted_iota(jnp.int32, (1, LANE), 1)
    small[0].wait()
    n_g = occ_buf.shape[1]
    occ_row[:, : occ_in.shape[1]] = occ_in[...]
    raw = occ_row[...]
    mine8 = (lane >= me_s * 8) & (lane < me_s * 8 + 8)
    for g in range(n_g):
        occ_buf[me_s, g : g + 1, :] = jnp.where(mine8, pltpu.roll(raw, me_s * 8 + (LANE - 8 * g) % LANE, 1), 0.0)
    for o in s_peers:
        remote(occ_buf.at[me_s], occ_buf.at[me_s], osend, orecv, number(o)).start()

    mine = local_copies(0, nt)
    more = local_copies(nt, 1)
    mine[0].wait()
    if_extra(lambda: more[0].wait())

    def clear(at, size):
        mil_buf[:, pl.ds(at, size)] = jnp.zeros((3, size), jnp.int32)
        psi_buf[:, :, :, :, pl.ds(at, size)] = jnp.zeros((*psi_buf.shape[:4], size), BF16)
        p_buf[:, :, :, pl.ds(at, size)] = jnp.zeros((2, na, PROJ, size), BF16)

    clear((nt + 1) * LANE, kp - (nt + 1) * LANE)

    @pl.when(jnp.logical_not(extra(me_s)))
    def _():
        clear(nt * LANE, LANE)

    small[1].wait()
    idx = [mil_buf[a : a + 1, :].astype(F32) for a in range(3)]
    co = [(idx[0] * lat_ref[0, a] + idx[1] * lat_ref[1, a] + idx[2] * lat_ref[2, a]) / MILLER for a in range(3)]
    iso = (co[0] * co[0] + co[1] * co[1] + co[2] * co[2]) / 3.0
    rows = list(co)
    for a, b in STRESS:
        prod = co[a] * co[b]
        rows.append(prod - iso if a == b else prod)
    for m, row in enumerate(rows):
        w_buf[m : m + 1, :] = row
    facc[...] = jnp.zeros_like(facc)
    sacc[...] = jnp.zeros_like(sacc)

    mine[1].wait()
    if_extra(lambda: more[1].wait())
    n_pc = len(p_chunks)
    up, down = number((1, 0, 0, 0, 0)), number((nz - 1, 0, 0, 0, 0))

    def plane(k):
        return pl.ds(pl.multiple_of(digits[0][k % nz] // n_r * n_s, n_s), n_s)

    def z_own(part, i):
        wait_recv(p_buf.at[:, pl.ds(0, n_s - 1), :, part], precv.at[i])
        ref = p_buf.at[:, plane(0), :, part]
        remote(ref, ref, zsend.at[0, i], zrecv.at[0, i], up).start()
        remote(ref, ref, zsend.at[1, i], zrecv.at[1, i], down).start()

    def z_next(part, i):
        wait_recv(p_buf.at[:, plane(0), :, part], zrecv.at[0, i])
        ref = p_buf.at[0, plane(-1), :, part]
        remote(ref, ref, zsend.at[2, i], zrecv.at[2, i], up).start()
        wait_recv(p_buf.at[:, plane(0), :, part], zrecv.at[1, i])
        ref = p_buf.at[1, plane(1), :, part]
        remote(ref, ref, zsend.at[3, i], zrecv.at[3, i], down).start()

    def z_end(part, i):
        wait_recv(p_buf.at[0, plane(0), :, part], zrecv.at[2, i])
        wait_recv(p_buf.at[1, plane(0), :, part], zrecv.at[3, i])

    def each_chunk(step):
        for i, chunk in enumerate(p_chunks):
            step(cols(chunk), i)
            if i == 0:
                if_extra(lambda: step(last, n_pc))

    each_chunk(z_own)
    each_chunk(z_next)

    mine[2].wait()
    if_extra(lambda: more[2].wait())
    for cp in small[2:]:
        cp.wait()
    kind = spec_ref[me_r]
    count = cnt_ref[me_r]
    act = (lax.broadcasted_iota(jnp.int32, (PROJ, PROJ), 0) < count) & (lax.broadcasted_iota(jnp.int32, (PROJ, PROJ), 1) < count)
    mat = jnp.where(act, coup_ref[kind], 0.0)
    front = lane < HALF
    z_done = [-1]

    def z_arrived(upto):
        while z_done[0] < n_pc - 1 and (z_done[0] < 0 or sum(p_chunks[z_done[0]]) < upto):
            z_done[0] += 1
            i = z_done[0]
            with jax.named_scope(f"wz{i}"):
                z_end(cols(p_chunks[i]), i)
            if i == 0:
                if_extra(lambda: z_end(last, n_pc))

    def gather_chunk(h, i):
        g0, gn, chunks = phases[h]
        acc = per[h][0]
        z_arrived(sum(chunks[i]))
        with jax.named_scope(f"wpsi{h}{i}"):
            wait_recv(psi_buf.at[:, pl.ds(g0, gn), pl.ds(0, n_s - 1), :, cols(chunks[i])], srecv.at[h, i])
        parts = [cols(chunks[i])]
        if i == 0:
            if_extra(lambda: wait_recv(psi_buf.at[:, pl.ds(g0, gn), pl.ds(0, n_s - 1), :, last], srecv.at[h, len(chunks)]))
            parts.append(pl.ds(nt * LANE, kp - nt * LANE))
        total = None if i == 0 else acc[...]
        for part in parts:
            rhs = jnp.concatenate([psi_buf[r, g, :, :, part].reshape(HALF, part.size) for g in range(g0, g0 + gn) for r in range(2)], axis=0)
            lhs = p_buf[:, :, :, part].reshape(2 * np_, part.size)
            term = lax.dot_general(lhs, rhs, (((1,), (1,)), ((), ())), preferred_element_type=F32)
            total = term if total is None else total + term
        acc[...] = total

    def reduce_start(h):
        acc, b_send, rs_buf = per[h][:3]
        for g in range(phases[h][1]):
            tile = pl.ds(g * LANE, LANE)
            low = pltpu.roll(acc[np_:, tile], HALF, 1)
            b_send[:, :, tile] = (acc[:np_, tile] + jnp.where(front, low, -low)).reshape(na, PROJ, LANE).astype(BF16)
        for o in r_peers:
            remote(b_send.at[number(o) - base], rs_buf.at[me_r], rsend.at[h], rrecv.at[h], number(o)).start()
        rs_buf[me_r] = b_send[me_r]

    def mix_and_spread(h):
        rs_buf, uv_buf = per[h][2:4]
        if h == 0:
            wait_recv(occ_buf.at[pl.ds(0, n_s - 1)], orecv)
        with jax.named_scope(f"rs_wait{h}"):
            wait_recv(rs_buf.at[pl.ds(0, n_r - 1)], rrecv.at[h])
        total = jnp.sum(rs_buf[...].astype(F32), axis=0)
        mixed = jnp.zeros_like(total)
        for i in range(PROJ):
            mixed = mixed + mat[:, i : i + 1] * total[i : i + 1, :]
        occ = jnp.sum(occ_buf[...], axis=0)
        occ = occ + pltpu.roll(occ, HALF, 1)
        for g in range(phases[h][1]):
            tile = pl.ds(g * LANE, LANE)
            at = phases[h][0] + g
            uv_buf[me_r, :, tile] = (mixed[:, g * LANE : (g + 1) * LANE] * occ[at : at + 1, :]).astype(BF16)
        for o in r_peers:
            remote(uv_buf.at[me_r], uv_buf.at[me_r], asend.at[h], arecv.at[h], number(o)).start()

    def collect(h):
        uv_buf, left = per[h][3:5]
        with jax.named_scope(f"ag_wait{h}"):
            wait_recv(uv_buf.at[pl.ds(0, n_r - 1)], arecv.at[h])
        uv = uv_buf[...].reshape(np_, phases[h][1] * LANE)
        left[:np_] = uv
        for g in range(phases[h][1]):
            tile = pl.ds(g * LANE, LANE)
            turned = pltpu.roll(uv[:, g * LANE : (g + 1) * LANE].astype(F32), HALF, 1)
            left[np_:, tile] = jnp.where(front, -turned, turned).astype(BF16)

    wide = 256

    def weighted(h, i):
        g0, gn, _ = phases[h]
        part = pl.ds(pl.multiple_of(i * wide, wide), wide)
        rhs = jnp.concatenate([psi_buf[r, g, :, :, part].reshape(HALF, wide) for g in range(g0, g0 + gn) for r in range(2)], axis=0)
        return part, jnp.dot(per[h][4][...], rhs, preferred_element_type=F32)

    def block(h, i, carry):
        part, y = weighted(h, i)
        y_re, y_im = y[:np_], y[np_:]
        p_re, p_im = p_wide[0, :, part], p_wide[1, :, part]
        e_im = (p_re * y_im - p_im * y_re).reshape(na, PROJ, wide)
        e_re = jnp.sum((p_re * y_re + p_im * y_im).reshape(na, PROJ, wide), axis=0)
        for a in range(3):
            t = e_im * w_buf[a : a + 1, part].reshape(1, 1, wide)
            facc[a] += t[:, :, :LANE] + t[:, :, LANE:]
        for m in range(6):
            t = e_re * w_buf[3 + m : 4 + m, part]
            sacc[m] += t[:, :LANE] + t[:, LANE:]
        return carry

    for i in range(len(phases[0][2])):
        gather_chunk(0, i)
    reduce_start(0)
    p_wide[...] = p_buf[...].reshape(2, np_, kp).astype(F32)
    if n_ph > 1:
        for i in range(len(phases[1][2])):
            gather_chunk(1, i)
        reduce_start(1)
        mix_and_spread(0)
    mix_and_spread(n_ph - 1)
    if n_ph > 1:
        collect(0)
        lax.fori_loop(0, kp // wide, functools.partial(block, 0), 0, unroll=UNROLL)
    collect(n_ph - 1)
    lax.fori_loop(0, kp // wide, functools.partial(block, n_ph - 1), 0, unroll=UNROLL)

    row = jnp.zeros((1, LANE), F32)
    for a in range(3):
        f = jnp.sum(facc[a], axis=1)
        f = jnp.concatenate([jnp.zeros((a * na, LANE), F32), f, jnp.zeros((LANE - (a + 1) * na, LANE), F32)][0 if a else 1 :], axis=0)
        row = row + jnp.sum(f.T, axis=0, keepdims=True)
    for m in range(6):
        row = row + jnp.where(lane == 3 * na + m, jnp.sum(sacc[m], keepdims=True), 0.0)
    tot[me] = row
    for o in all_peers:
        remote(tot.at[me], tot.at[me], fsend, frecv, number(o)).start()
    wait_recv(tot.at[pl.ds(0, n_all - 1)], frecv)
    out_ref[...] = jnp.sum(tot[...], axis=0)

    for i, chunk in enumerate(p_chunks):
        wait_send(p_buf.at[:, pl.ds(0, n_s - 1), :, cols(chunk)], psend.at[i])

    def z_sent(part, i):
        for k in range(4):
            wait_send(p_buf.at[:, plane(0), :, part] if k < 2 else p_buf.at[0, plane(0), :, part], zsend.at[k, i])

    each_chunk(z_sent)
    for h, (g0, gn, chunks) in enumerate(phases):
        for i, chunk in enumerate(chunks):
            wait_send(psi_buf.at[:, pl.ds(g0, gn), pl.ds(0, n_s - 1), :, cols(chunk)], ssend.at[h, i])
        wait_send(per[h][2].at[pl.ds(0, n_r - 1)], rsend.at[h])
        wait_send(per[h][3].at[pl.ds(0, n_r - 1)], asend.at[h])
    for o in s_peers:

        @pl.when(extra(slice_of(o)))
        def _():
            wait_send(p_buf.at[:, 0, :, last], psend.at[n_pc])
            for h, (g0, gn, chunks) in enumerate(phases):
                wait_send(psi_buf.at[:, pl.ds(g0, gn), 0, :, last], ssend.at[h, len(chunks)])

    wait_send(occ_buf.at[pl.ds(0, n_s - 1)], osend)
    wait_send(tot.at[pl.ds(0, n_all - 1)], fsend)


def finish(dims, na, scales, row_ref, force_ref, stress_ref):
    res = row_ref[...]
    beta = (lax.axis_index("z") * dims[1] + lax.axis_index("yh")) * dims[2] + lax.axis_index("x")
    lane = lax.broadcasted_iota(jnp.int32, (1, LANE), 1)
    own = [jnp.sum(jnp.where(lane == a * na + beta, res, 0.0), axis=1, keepdims=True) for a in range(3)]
    force_ref[...] = jnp.where(lane[:, :3] == 0, own[0], jnp.where(lane[:, :3] == 1, own[1], own[2])) * scales[0]
    i0 = lax.broadcasted_iota(jnp.int32, (3, 3), 0)
    i1 = lax.broadcasted_iota(jnp.int32, (3, 3), 1)
    st = jnp.zeros((3, 3), F32)
    for m, (a, b) in enumerate(STRESS):
        val = jnp.sum(jnp.where(lane == 3 * na + m, res, 0.0), axis=1, keepdims=True)
        hit = ((i0 == a) & (i1 == b)) | ((i0 == b) & (i1 == a))
        st = st + jnp.where(hit, val, 0.0)
    stress_ref[...] = st * scales[1]


def cut(total, wants):
    chunks, at = [], 0
    for n in wants:
        if at + n < total:
            chunks.append((at, n))
            at += n
    chunks.append((at, total - at))
    return tuple(chunks)


UNROLL = 5
P_CUT = (4, 6)
SETS = ((2, (10,)), (2, (8, 8)))


def body(dims, psi, proj, miller, lattice, occupation, species, proj_count, coupling):
    nz, nyh, nx, nyl, nc = dims
    n_s = nyh * nx
    n_r = n_s * nyl * nc
    bands = psi.shape[1]
    n_g = bands // 8
    tiles = psi.shape[2] // LANE
    atoms = species.shape[0]
    nt = tiles // n_s
    p_chunks = cut(nt, P_CUT)
    phases, at = [], 0
    for gn, wants in SETS:
        phases.append((at, gn, cut(nt, wants)))
        at += gn
    n_ph = len(phases)
    most = max(len(chunks) for _, _, chunks in phases) + 1
    n_pc = len(p_chunks) + 1
    kp = -(-(nt + 1) * LANE // 256) * 256
    band_total = bands * n_s * nz
    scales = (2.0 / (PROJ * math.sqrt(band_total)), 1.0 / (PROJ * math.sqrt(atoms * band_total)))
    any_spec = pl.BlockSpec(memory_space=pl.ANY)
    vmem = pl.BlockSpec(memory_space=pltpu.VMEM)
    dma = pltpu.SemaphoreType.DMA
    scratch = [
        pltpu.VMEM((2, n_g, n_s, 8, kp), BF16),
        pltpu.VMEM((2, atoms, PROJ, kp), BF16),
        pltpu.VMEM((3, kp), jnp.int32),
        pltpu.VMEM((n_s, n_g, LANE), F32),
        pltpu.VMEM((16, kp), F32),
        pltpu.SMEM((3, 3), F32), pltpu.SMEM(species.shape, jnp.int32), pltpu.SMEM(species.shape, jnp.int32),
        pltpu.VMEM(coupling.shape, F32), pltpu.VMEM((1, LANE), F32), pltpu.VMEM((1, bands), F32),
        pltpu.VMEM((2, atoms * PROJ, kp), F32),
        pltpu.VMEM((3, atoms, PROJ, LANE), F32),
        pltpu.VMEM((6, PROJ, LANE), F32),
        pltpu.VMEM((nz * n_r, 1, LANE), F32),
    ]
    for _, gn, _ in phases:
        width = gn * LANE
        scratch += [
            pltpu.VMEM((2 * atoms * PROJ, width), F32),
            pltpu.VMEM((atoms, PROJ, width), BF16),
            pltpu.VMEM((n_r, PROJ, width), BF16),
            pltpu.VMEM((n_r, PROJ, width), BF16),
            pltpu.VMEM((2 * atoms * PROJ, width), BF16),
            ]
    scratch += [dma((8,)), *[dma((n_pc,))] * 2, *[dma((4, n_pc))] * 2, dma, dma, *[dma((n_ph, most))] * 2, *[dma((n_ph,))] * 4, dma, dma]
    row = pl.pallas_call(
        functools.partial(kernel, dims, nt, tiles, p_chunks, tuple(phases)),
        out_shape=pltpu.VMEM((1, LANE), F32),
        in_specs=[any_spec] * 8,
        out_specs=vmem,
        scratch_shapes=scratch,
        compiler_params=pltpu.CompilerParams(collective_id=0, has_side_effects=True, vmem_limit_bytes=58 << 20),
        name="plane_kernel",
    )(psi.reshape(2, n_g, 8, psi.shape[2]), proj, miller, lattice, occupation[None], species, proj_count, coupling)
    force, stress = pl.pallas_call(
        functools.partial(finish, dims, atoms, scales),
        out_shape=(jax.ShapeDtypeStruct((1, 3), F32), jax.ShapeDtypeStruct((3, 3), F32)),
        in_specs=[vmem],
        out_specs=(vmem, vmem),
        name="finish",
    )(pltpu.with_memory_space_constraint(row, pltpu.VMEM))
    return force.T, stress


def solution(mesh, dims=(4, 2, 4, 2, 2)):
    finer = Mesh(mesh.devices.reshape(dims), AXES)
    band, gvec = ("z", "yh", "x"), ("yl", "core")
    in_specs = (P(None, band, gvec), P(None, band, gvec), P(None, gvec), P(), P(band), P(), P(), P())
    return jax.shard_map(functools.partial(body, dims), mesh=finer, in_specs=in_specs, out_specs=(P(None, band), P()), check_vma=False)
```

```python
import functools
import itertools
import math

import jax
import jax.numpy as jnp
from jax import lax
from jax.experimental import pallas as pl
from jax.experimental.pallas import tpu as pltpu
from jax.sharding import Mesh
from jax.sharding import PartitionSpec as P

PROJ = 8
MILLER = 24.0
LANE = 128
HALF = 64
LOGICAL = pl.DeviceIdType.LOGICAL
F32 = jnp.float32
BF16 = jnp.bfloat16
AXES = ("z", "yh", "x", "yl", "core")
STRESS = ((0, 0), (1, 1), (2, 2), (0, 1), (0, 2), (1, 2))


def kernel(
    dims, nt, tiles, p_chunks, phases,
    psi_hbm, proj_hbm, miller_hbm, lat_hbm, occ_hbm, spec_hbm, cnt_hbm, coup_hbm,
    out_ref,
    psi_buf, p_buf, mil_buf, occ_buf, w_buf, lat_ref, spec_ref, cnt_ref, coup_ref, occ_row, occ_in, p_wide, facc, sacc, tot,
    *rest,
):
    n_ph = len(phases)
    per = [rest[i * 5 : i * 5 + 5] for i in range(n_ph)]
    loc_sem, psend, precv, zsend, zrecv, osend, orecv, ssend, srecv, rsend, rrecv, asend, arecv, fsend, frecv = rest[5 * n_ph :]
    nz, nyh, nx, nyl, nc = dims
    n_s = nyh * nx
    n_r = n_s * nyl * nc
    n_all = nz * n_r
    z, yh, x, yl, c = (lax.axis_index(a) for a in AXES)
    me_s = yh * nx + x
    me_r = me_s * (nyl * nc) + yl * nc + c
    me = z * n_r + me_r
    beta = z * n_s + me_s
    na = p_buf.shape[1]
    np_ = na * PROJ
    kp = w_buf.shape[1]

    strides = (n_r, nx * nyl * nc, nyl * nc, nc, 1)
    digits = []
    for at, n, stride in zip((z, yh, x, yl, c), dims, strides):
        digits.append([jnp.where(at + k >= n, at + k - n, at + k) * stride if k else at * stride for k in range(n)])

    def hops(offset):
        dz, a, b, d, e = offset
        return min(dz, nz - dz) + min(b, nx - b) + (2 if a and not d else 1 if a or d else 0)

    def peers(free):
        spans = [range(n) if f else (0,) for n, f in zip(dims, free)]
        offsets = [o for o in itertools.product(*spans) if any(o)]
        return sorted(offsets, key=lambda o: -hops(o))

    def number(offset):
        return sum(digits[i][k] for i, k in enumerate(offset))

    s_peers = peers((0, 1, 1, 0, 0))
    r_peers = peers((0, 1, 1, 1, 1))
    z_peers = peers((1, 0, 0, 0, 0))
    all_peers = peers((1, 1, 1, 1, 1))
    base = digits[0][0]

    def slice_of(offset):
        return (digits[1][offset[1]] + digits[2][offset[2]]) // (nyl * nc)

    def first_tile(q):
        return (q * tiles + (n_s // 2) * c + (n_s // 4) * yl) // n_s

    def extra(q):
        return first_tile(q + 1) - first_tile(q) > nt

    def remote(src, dst, ssem, rsem, where):
        return pltpu.make_async_remote_copy(src, dst, ssem, rsem, device_id=where, device_id_type=LOGICAL)

    def wait_recv(ref, sem):
        remote(ref, ref, sem, sem, number(s_peers[0])).wait_recv()

    def wait_send(ref, sem):
        remote(ref, ref, sem, sem, number(s_peers[0])).wait_send()

    my_off = pl.multiple_of(first_tile(me_s) * LANE, LANE)
    if_extra = pl.when(extra(me_s))
    last = pl.ds(nt * LANE, LANE)

    def cols(chunk):
        return pl.ds(chunk[0] * LANE, chunk[1] * LANE)

    def local_copies(t0, tn):
        here = pl.ds(pl.multiple_of(my_off + t0 * LANE, LANE), tn * LANE)
        there = pl.ds(t0 * LANE, tn * LANE)
        return [pltpu.make_async_copy(miller_hbm.at[:, here], mil_buf.at[:, there], loc_sem.at[0]),
                pltpu.make_async_copy(proj_hbm.at[:, :, here], p_buf.at[:, beta, :, there], loc_sem.at[1]),
                pltpu.make_async_copy(psi_hbm.at[:, :, :, here], psi_buf.at[:, :, me_s, :, there], loc_sem.at[2])]

    small = [pltpu.make_async_copy(a, b, loc_sem.at[3 + n]) for n, (a, b) in enumerate((
        (occ_hbm, occ_in), (lat_hbm, lat_ref), (spec_hbm, spec_ref), (cnt_hbm, cnt_ref), (coup_hbm, coup_ref)))]

    bar = pltpu.get_barrier_semaphore()
    for o in sorted(z_peers + r_peers, key=lambda o: -hops(o)):
        pl.semaphore_signal(bar, 1, device_id=number(o), device_id_type=LOGICAL)
    occ_row[...] = jnp.zeros_like(occ_row)
    for cp in small + local_copies(0, nt):
        cp.start()

    @if_extra
    def _():
        for cp in local_copies(nt, 1):
            cp.start()

    pl.semaphore_wait(bar, n_r - 1 + nz - 1)

    def send_slices(src, dst_of, chunks, ssem, rsem):
        for i, (t0, tn) in enumerate(chunks):
            for o in s_peers:
                q, where = slice_of(o), number(o)
                off = pl.multiple_of((first_tile(q) + t0) * LANE, LANE)
                remote(src(pl.ds(off, tn * LANE)), dst_of(cols((t0, tn))), ssem(i), rsem(i), where).start()
                if i == 0:

                    @pl.when(extra(q))
                    def _():
                        end = pl.multiple_of((first_tile(q) + nt) * LANE, LANE)
                        remote(src(pl.ds(end, LANE)), dst_of(last), ssem(len(chunks)), rsem(len(chunks)), where).start()

    send_slices(lambda part: proj_hbm.at[:, :, part], lambda part: p_buf.at[:, beta, :, part], p_chunks, lambda i: psend.at[i], lambda i: precv.at[i])
    for h, (g0, gn, chunks) in enumerate(phases):
        send_slices(lambda part: psi_hbm.at[:, pl.ds(g0, gn), :, part], lambda part: psi_buf.at[:, pl.ds(g0, gn), me_s, :, part],
                    chunks, lambda i: ssend.at[h, i], lambda i: srecv.at[h, i])

    lane = lax.broadcasted_iota(jnp.int32, (1, LANE), 1)
    small[0].wait()
    n_g = occ_buf.shape[1]
    occ_row[:, : occ_in.shape[1]] = occ_in[...]
    raw = occ_row[...]
    mine8 = (lane >= me_s * 8) & (lane < me_s * 8 + 8)
    for g in range(n_g):
        occ_buf[me_s, g : g + 1, :] = jnp.where(mine8, pltpu.roll(raw, me_s * 8 + (LANE - 8 * g) % LANE, 1), 0.0)
    for o in s_peers:
        remote(occ_buf.at[me_s], occ_buf.at[me_s], osend, orecv, number(o)).start()

    mine = local_copies(0, nt)
    more = local_copies(nt, 1)
    mine[0].wait()
    if_extra(lambda: more[0].wait())

    def clear(at, size):
        mil_buf[:, pl.ds(at, size)] = jnp.zeros((3, size), jnp.int32)
        psi_buf[:, :, :, :, pl.ds(at, size)] = jnp.zeros((*psi_buf.shape[:4], size), BF16)
        p_buf[:, :, :, pl.ds(at, size)] = jnp.zeros((2, na, PROJ, size), BF16)

    clear((nt + 1) * LANE, kp - (nt + 1) * LANE)

    @pl.when(jnp.logical_not(extra(me_s)))
    def _():
        clear(nt * LANE, LANE)

    small[1].wait()
    idx = [mil_buf[a : a + 1, :].astype(F32) for a in range(3)]
    co = [(idx[0] * lat_ref[0, a] + idx[1] * lat_ref[1, a] + idx[2] * lat_ref[2, a]) / MILLER for a in range(3)]
    iso = (co[0] * co[0] + co[1] * co[1] + co[2] * co[2]) / 3.0
    rows = list(co)
    for a, b in STRESS:
        prod = co[a] * co[b]
        rows.append(prod - iso if a == b else prod)
    for m, row in enumerate(rows):
        w_buf[m : m + 1, :] = row
    facc[...] = jnp.zeros_like(facc)
    sacc[...] = jnp.zeros_like(sacc)

    mine[1].wait()
    if_extra(lambda: more[1].wait())
    n_pc = len(p_chunks)
    up, down = number((1, 0, 0, 0, 0)), number((nz - 1, 0, 0, 0, 0))

    def plane(k):
        return pl.ds(pl.multiple_of(digits[0][k % nz] // n_r * n_s, n_s), n_s)

    def z_own(part, i):
        wait_recv(p_buf.at[:, pl.ds(0, n_s - 1), :, part], precv.at[i])
        ref = p_buf.at[:, plane(0), :, part]
        remote(ref, ref, zsend.at[0, i], zrecv.at[0, i], up).start()
        remote(ref, ref, zsend.at[1, i], zrecv.at[1, i], down).start()

    def z_next(part, i):
        wait_recv(p_buf.at[:, plane(0), :, part], zrecv.at[0, i])
        ref = p_buf.at[0, plane(-1), :, part]
        remote(ref, ref, zsend.at[2, i], zrecv.at[2, i], up).start()
        wait_recv(p_buf.at[:, plane(0), :, part], zrecv.at[1, i])
        ref = p_buf.at[1, plane(1), :, part]
        remote(ref, ref, zsend.at[3, i], zrecv.at[3, i], down).start()

    def z_end(part, i):
        wait_recv(p_buf.at[0, plane(0), :, part], zrecv.at[2, i])
        wait_recv(p_buf.at[1, plane(0), :, part], zrecv.at[3, i])

    def each_chunk(step):
        for i, chunk in enumerate(p_chunks):
            step(cols(chunk), i)
            if i == 0:
                if_extra(lambda: step(last, n_pc))

    each_chunk(z_own)
    each_chunk(z_next)

    mine[2].wait()
    if_extra(lambda: more[2].wait())
    for cp in small[2:]:
        cp.wait()
    kind = spec_ref[me_r]
    count = cnt_ref[me_r]
    act = (lax.broadcasted_iota(jnp.int32, (PROJ, PROJ), 0) < count) & (lax.broadcasted_iota(jnp.int32, (PROJ, PROJ), 1) < count)
    mat = jnp.where(act, coup_ref[kind], 0.0)
    front = lane < HALF
    z_done = [-1]

    def z_arrived(upto):
        while z_done[0] < n_pc - 1 and (z_done[0] < 0 or sum(p_chunks[z_done[0]]) < upto):
            z_done[0] += 1
            i = z_done[0]
            with jax.named_scope(f"wz{i}"):
                z_end(cols(p_chunks[i]), i)
            if i == 0:
                if_extra(lambda: z_end(last, n_pc))

    def gather_chunk(h, i):
        g0, gn, chunks = phases[h]
        acc = per[h][0]
        z_arrived(sum(chunks[i]))
        with jax.named_scope(f"wpsi{h}{i}"):
            wait_recv(psi_buf.at[:, pl.ds(g0, gn), pl.ds(0, n_s - 1), :, cols(chunks[i])], srecv.at[h, i])
        parts = [cols(chunks[i])]
        if i == 0:
            if_extra(lambda: wait_recv(psi_buf.at[:, pl.ds(g0, gn), pl.ds(0, n_s - 1), :, last], srecv.at[h, len(chunks)]))
            parts.append(pl.ds(nt * LANE, kp - nt * LANE))
        total = None if i == 0 else acc[...]
        for part in parts:
            rhs = jnp.concatenate([psi_buf[r, g, :, :, part].reshape(HALF, part.size) for g in range(g0, g0 + gn) for r in range(2)], axis=0)
            lhs = p_buf[:, :, :, part].reshape(2 * np_, part.size)
            term = lax.dot_general(lhs, rhs, (((1,), (1,)), ((), ())), preferred_element_type=F32)
            total = term if total is None else total + term
        acc[...] = total

    def reduce_start(h):
        acc, b_send, rs_buf = per[h][:3]
        for g in range(phases[h][1]):
            tile = pl.ds(g * LANE, LANE)
            low = pltpu.roll(acc[np_:, tile], HALF, 1)
            b_send[:, :, tile] = (acc[:np_, tile] + jnp.where(front, low, -low)).reshape(na, PROJ, LANE).astype(BF16)
        for o in r_peers:
            remote(b_send.at[number(o) - base], rs_buf.at[me_r], rsend.at[h], rrecv.at[h], number(o)).start()
        rs_buf[me_r] = b_send[me_r]

    def mix_and_spread(h):
        rs_buf, uv_buf = per[h][2:4]
        if h == 0:
            wait_recv(occ_buf.at[pl.ds(0, n_s - 1)], orecv)
        with jax.named_scope(f"rs_wait{h}"):
            wait_recv(rs_buf.at[pl.ds(0, n_r - 1)], rrecv.at[h])
        total = jnp.sum(rs_buf[...].astype(F32), axis=0)
        mixed = jnp.zeros_like(total)
        for i in range(PROJ):
            mixed = mixed + mat[:, i : i + 1] * total[i : i + 1, :]
        occ = jnp.sum(occ_buf[...], axis=0)
        occ = occ + pltpu.roll(occ, HALF, 1)
        for g in range(phases[h][1]):
            tile = pl.ds(g * LANE, LANE)
            at = phases[h][0] + g
            uv_buf[me_r, :, tile] = (mixed[:, g * LANE : (g + 1) * LANE] * occ[at : at + 1, :]).astype(BF16)
        for o in r_peers:
            remote(uv_buf.at[me_r], uv_buf.at[me_r], asend.at[h], arecv.at[h], number(o)).start()

    def collect(h):
        uv_buf, left = per[h][3:5]
        with jax.named_scope(f"ag_wait{h}"):
            wait_recv(uv_buf.at[pl.ds(0, n_r - 1)], arecv.at[h])
        uv = uv_buf[...].reshape(np_, phases[h][1] * LANE)
        left[:np_] = uv
        for g in range(phases[h][1]):
            tile = pl.ds(g * LANE, LANE)
            turned = pltpu.roll(uv[:, g * LANE : (g + 1) * LANE].astype(F32), HALF, 1)
            left[np_:, tile] = jnp.where(front, -turned, turned).astype(BF16)

    wide = 256

    def weighted(h, i):
        g0, gn, _ = phases[h]
        part = pl.ds(pl.multiple_of(i * wide, wide), wide)
        rhs = jnp.concatenate([psi_buf[r, g, :, :, part].reshape(HALF, wide) for g in range(g0, g0 + gn) for r in range(2)], axis=0)
        return part, jnp.dot(per[h][4][...], rhs, preferred_element_type=F32)

    def block(h, i, carry):
        part, y = weighted(h, i)
        y_re, y_im = y[:np_], y[np_:]
        p_re, p_im = p_wide[0, :, part], p_wide[1, :, part]
        e_im = (p_re * y_im - p_im * y_re).reshape(na, PROJ, wide)
        e_re = jnp.sum((p_re * y_re + p_im * y_im).reshape(na, PROJ, wide), axis=0)
        for a in range(3):
            t = e_im * w_buf[a : a + 1, part].reshape(1, 1, wide)
            facc[a] += t[:, :, :LANE] + t[:, :, LANE:]
        for m in range(6):
            t = e_re * w_buf[3 + m : 4 + m, part]
            sacc[m] += t[:, :LANE] + t[:, LANE:]
        return carry

    for i in range(len(phases[0][2])):
        gather_chunk(0, i)
    reduce_start(0)
    p_wide[...] = p_buf[...].reshape(2, np_, kp).astype(F32)
    if n_ph > 1:
        for i in range(len(phases[1][2])):
            gather_chunk(1, i)
        reduce_start(1)
        mix_and_spread(0)
    mix_and_spread(n_ph - 1)
    if n_ph > 1:
        collect(0)
        lax.fori_loop(0, kp // wide, functools.partial(block, 0), 0, unroll=UNROLL)
    collect(n_ph - 1)
    lax.fori_loop(0, kp // wide, functools.partial(block, n_ph - 1), 0, unroll=UNROLL)

    row = jnp.zeros((1, LANE), F32)
    for a in range(3):
        f = jnp.sum(facc[a], axis=1)
        f = jnp.concatenate([jnp.zeros((a * na, LANE), F32), f, jnp.zeros((LANE - (a + 1) * na, LANE), F32)][0 if a else 1 :], axis=0)
        row = row + jnp.sum(f.T, axis=0, keepdims=True)
    for m in range(6):
        row = row + jnp.where(lane == 3 * na + m, jnp.sum(sacc[m], keepdims=True), 0.0)
    tot[me] = row
    for o in all_peers:
        remote(tot.at[me], tot.at[me], fsend, frecv, number(o)).start()
    wait_recv(tot.at[pl.ds(0, n_all - 1)], frecv)
    out_ref[...] = jnp.sum(tot[...], axis=0)

    for i, chunk in enumerate(p_chunks):
        wait_send(p_buf.at[:, pl.ds(0, n_s - 1), :, cols(chunk)], psend.at[i])

    def z_sent(part, i):
        for k in range(4):
            wait_send(p_buf.at[:, plane(0), :, part] if k < 2 else p_buf.at[0, plane(0), :, part], zsend.at[k, i])

    each_chunk(z_sent)
    for h, (g0, gn, chunks) in enumerate(phases):
        for i, chunk in enumerate(chunks):
            wait_send(psi_buf.at[:, pl.ds(g0, gn), pl.ds(0, n_s - 1), :, cols(chunk)], ssend.at[h, i])
        wait_send(per[h][2].at[pl.ds(0, n_r - 1)], rsend.at[h])
        wait_send(per[h][3].at[pl.ds(0, n_r - 1)], asend.at[h])
    for o in s_peers:

        @pl.when(extra(slice_of(o)))
        def _():
            wait_send(p_buf.at[:, 0, :, last], psend.at[n_pc])
            for h, (g0, gn, chunks) in enumerate(phases):
                wait_send(psi_buf.at[:, pl.ds(g0, gn), 0, :, last], ssend.at[h, len(chunks)])

    wait_send(occ_buf.at[pl.ds(0, n_s - 1)], osend)
    wait_send(tot.at[pl.ds(0, n_all - 1)], fsend)


def finish(dims, na, scales, row_ref, force_ref, stress_ref):
    res = row_ref[...]
    beta = (lax.axis_index("z") * dims[1] + lax.axis_index("yh")) * dims[2] + lax.axis_index("x")
    lane = lax.broadcasted_iota(jnp.int32, (1, LANE), 1)
    own = [jnp.sum(jnp.where(lane == a * na + beta, res, 0.0), axis=1, keepdims=True) for a in range(3)]
    force_ref[...] = jnp.where(lane[:, :3] == 0, own[0], jnp.where(lane[:, :3] == 1, own[1], own[2])) * scales[0]
    i0 = lax.broadcasted_iota(jnp.int32, (3, 3), 0)
    i1 = lax.broadcasted_iota(jnp.int32, (3, 3), 1)
    st = jnp.zeros((3, 3), F32)
    for m, (a, b) in enumerate(STRESS):
        val = jnp.sum(jnp.where(lane == 3 * na + m, res, 0.0), axis=1, keepdims=True)
        hit = ((i0 == a) & (i1 == b)) | ((i0 == b) & (i1 == a))
        st = st + jnp.where(hit, val, 0.0)
    stress_ref[...] = st * scales[1]


def cut(total, wants):
    chunks, at = [], 0
    for n in wants:
        if at + n < total:
            chunks.append((at, n))
            at += n
    chunks.append((at, total - at))
    return tuple(chunks)


UNROLL = 5
P_CUT = (4, 6)
SETS = ((2, (10,)), (2, (8, 8)))


def body(dims, psi, proj, miller, lattice, occupation, species, proj_count, coupling):
    nz, nyh, nx, nyl, nc = dims
    n_s = nyh * nx
    n_r = n_s * nyl * nc
    bands = psi.shape[1]
    n_g = bands // 8
    tiles = psi.shape[2] // LANE
    atoms = species.shape[0]
    nt = tiles // n_s
    p_chunks = cut(nt, P_CUT)
    phases, at = [], 0
    for gn, wants in SETS:
        phases.append((at, gn, cut(nt, wants)))
        at += gn
    n_ph = len(phases)
    most = max(len(chunks) for _, _, chunks in phases) + 1
    n_pc = len(p_chunks) + 1
    kp = -(-(nt + 1) * LANE // 256) * 256
    band_total = bands * n_s * nz
    scales = (2.0 / (PROJ * math.sqrt(band_total)), 1.0 / (PROJ * math.sqrt(atoms * band_total)))
    any_spec = pl.BlockSpec(memory_space=pl.ANY)
    vmem = pl.BlockSpec(memory_space=pltpu.VMEM)
    dma = pltpu.SemaphoreType.DMA
    scratch = [
        pltpu.VMEM((2, n_g, n_s, 8, kp), BF16),
        pltpu.VMEM((2, atoms, PROJ, kp), BF16),
        pltpu.VMEM((3, kp), jnp.int32),
        pltpu.VMEM((n_s, n_g, LANE), F32),
        pltpu.VMEM((16, kp), F32),
        pltpu.SMEM((3, 3), F32), pltpu.SMEM(species.shape, jnp.int32), pltpu.SMEM(species.shape, jnp.int32),
        pltpu.VMEM(coupling.shape, F32), pltpu.VMEM((1, LANE), F32), pltpu.VMEM((1, bands), F32),
        pltpu.VMEM((2, atoms * PROJ, kp), F32),
        pltpu.VMEM((3, atoms, PROJ, LANE), F32),
        pltpu.VMEM((6, PROJ, LANE), F32),
        pltpu.VMEM((nz * n_r, 1, LANE), F32),
    ]
    for _, gn, _ in phases:
        width = gn * LANE
        scratch += [
            pltpu.VMEM((2 * atoms * PROJ, width), F32),
            pltpu.VMEM((atoms, PROJ, width), BF16),
            pltpu.VMEM((n_r, PROJ, width), BF16),
            pltpu.VMEM((n_r, PROJ, width), BF16),
            pltpu.VMEM((2 * atoms * PROJ, width), BF16),
            ]
    scratch += [dma((8,)), *[dma((n_pc,))] * 2, *[dma((4, n_pc))] * 2, dma, dma, *[dma((n_ph, most))] * 2, *[dma((n_ph,))] * 4, dma, dma]
    row = pl.pallas_call(
        functools.partial(kernel, dims, nt, tiles, p_chunks, tuple(phases)),
        out_shape=pltpu.VMEM((1, LANE), F32),
        in_specs=[any_spec] * 8,
        out_specs=vmem,
        scratch_shapes=scratch,
        compiler_params=pltpu.CompilerParams(collective_id=0, has_side_effects=True, vmem_limit_bytes=58 << 20),
        name="plane_kernel",
    )(psi.reshape(2, n_g, 8, psi.shape[2]), proj, miller, lattice, occupation[None], species, proj_count, coupling)
    force, stress = pl.pallas_call(
        functools.partial(finish, dims, atoms, scales),
        out_shape=(jax.ShapeDtypeStruct((1, 3), F32), jax.ShapeDtypeStruct((3, 3), F32)),
        in_specs=[vmem],
        out_specs=(vmem, vmem),
        name="finish",
    )(pltpu.with_memory_space_constraint(row, pltpu.VMEM))
    return force.T, stress


def solution(mesh, dims=(4, 2, 4, 2, 2)):
    finer = Mesh(mesh.devices.reshape(dims), AXES)
    band, gvec = ("z", "yh", "x"), ("yl", "core")
    in_specs = (P(None, band, gvec), P(None, band, gvec), P(None, gvec), P(), P(band), P(), P(), P())
    return jax.shard_map(functools.partial(body, dims), mesh=finer, in_specs=in_specs, out_specs=(P(None, band), P()), check_vma=False)
```

```python
import functools
import itertools
import math

import jax
import jax.numpy as jnp
from jax import lax
from jax.experimental import pallas as pl
from jax.experimental.pallas import tpu as pltpu
from jax.sharding import Mesh
from jax.sharding import PartitionSpec as P

PROJ = 8
MILLER = 24.0
LANE = 128
HALF = 64
LOGICAL = pl.DeviceIdType.LOGICAL
F32 = jnp.float32
BF16 = jnp.bfloat16
AXES = ("z", "yh", "x", "yl", "core")
STRESS = ((0, 0), (1, 1), (2, 2), (0, 1), (0, 2), (1, 2))


def kernel(
    dims, nt, tiles, p_chunks, phases,
    psi_hbm, proj_hbm, miller_hbm, lat_hbm, occ_hbm, spec_hbm, cnt_hbm, coup_hbm,
    out_ref,
    psi_buf, p_buf, mil_buf, occ_buf, w_buf, lat_ref, spec_ref, cnt_ref, coup_ref, occ_row, occ_in, p_wide, facc, sacc, tot,
    *rest,
):
    n_ph = len(phases)
    per = [rest[i * 5 : i * 5 + 5] for i in range(n_ph)]
    loc_sem, psend, precv, zsend, zrecv, osend, orecv, ssend, srecv, rsend, rrecv, asend, arecv, fsend, frecv = rest[5 * n_ph :]
    nz, nyh, nx, nyl, nc = dims
    n_s = nyh * nx
    n_r = n_s * nyl * nc
    n_all = nz * n_r
    z, yh, x, yl, c = (lax.axis_index(a) for a in AXES)
    me_s = yh * nx + x
    me_r = me_s * (nyl * nc) + yl * nc + c
    me = z * n_r + me_r
    beta = z * n_s + me_s
    na = p_buf.shape[1]
    np_ = na * PROJ
    kp = w_buf.shape[1]

    strides = (n_r, nx * nyl * nc, nyl * nc, nc, 1)
    digits = []
    for at, n, stride in zip((z, yh, x, yl, c), dims, strides):
        digits.append([jnp.where(at + k >= n, at + k - n, at + k) * stride if k else at * stride for k in range(n)])

    def hops(offset):
        dz, a, b, d, e = offset
        return min(dz, nz - dz) + min(b, nx - b) + (2 if a and not d else 1 if a or d else 0)

    def peers(free):
        spans = [range(n) if f else (0,) for n, f in zip(dims, free)]
        offsets = [o for o in itertools.product(*spans) if any(o)]
        return sorted(offsets, key=lambda o: -hops(o))

    def number(offset):
        return sum(digits[i][k] for i, k in enumerate(offset))

    s_peers = peers((0, 1, 1, 0, 0))
    r_peers = peers((0, 1, 1, 1, 1))
    z_peers = peers((1, 0, 0, 0, 0))
    all_peers = peers((1, 1, 1, 1, 1))
    base = digits[0][0]

    def slice_of(offset):
        return (digits[1][offset[1]] + digits[2][offset[2]]) // (nyl * nc)

    def first_tile(q):
        return (q * tiles + (n_s // 2) * c + (n_s // 4) * yl) // n_s

    def extra(q):
        return first_tile(q + 1) - first_tile(q) > nt

    def remote(src, dst, ssem, rsem, where):
        return pltpu.make_async_remote_copy(src, dst, ssem, rsem, device_id=where, device_id_type=LOGICAL)

    def wait_recv(ref, sem):
        remote(ref, ref, sem, sem, number(s_peers[0])).wait_recv()

    def wait_send(ref, sem):
        remote(ref, ref, sem, sem, number(s_peers[0])).wait_send()

    my_off = pl.multiple_of(first_tile(me_s) * LANE, LANE)
    if_extra = pl.when(extra(me_s))
    last = pl.ds(nt * LANE, LANE)

    def cols(chunk):
        return pl.ds(chunk[0] * LANE, chunk[1] * LANE)

    def local_copies(t0, tn):
        here = pl.ds(pl.multiple_of(my_off + t0 * LANE, LANE), tn * LANE)
        there = pl.ds(t0 * LANE, tn * LANE)
        return [pltpu.make_async_copy(miller_hbm.at[:, here], mil_buf.at[:, there], loc_sem.at[0]),
                pltpu.make_async_copy(proj_hbm.at[:, :, here], p_buf.at[:, beta, :, there], loc_sem.at[1]),
                pltpu.make_async_copy(psi_hbm.at[:, :, :, here], psi_buf.at[:, :, me_s, :, there], loc_sem.at[2])]

    small = [pltpu.make_async_copy(a, b, loc_sem.at[3 + n]) for n, (a, b) in enumerate((
        (occ_hbm, occ_in), (lat_hbm, lat_ref), (spec_hbm, spec_ref), (cnt_hbm, cnt_ref), (coup_hbm, coup_ref)))]

    bar = pltpu.get_barrier_semaphore()
    for o in sorted(z_peers + r_peers, key=lambda o: -hops(o)):
        pl.semaphore_signal(bar, 1, device_id=number(o), device_id_type=LOGICAL)
    occ_row[...] = jnp.zeros_like(occ_row)
    for cp in small + local_copies(0, nt):
        cp.start()

    @if_extra
    def _():
        for cp in local_copies(nt, 1):
            cp.start()

    pl.semaphore_wait(bar, n_r - 1 + nz - 1)

    def send_slices(src, dst_of, chunks, ssem, rsem):
        for i, (t0, tn) in enumerate(chunks):
            for o in s_peers:
                q, where = slice_of(o), number(o)
                off = pl.multiple_of((first_tile(q) + t0) * LANE, LANE)
                remote(src(pl.ds(off, tn * LANE)), dst_of(cols((t0, tn))), ssem(i), rsem(i), where).start()
                if i == 0:

                    @pl.when(extra(q))
                    def _():
                        end = pl.multiple_of((first_tile(q) + nt) * LANE, LANE)
                        remote(src(pl.ds(end, LANE)), dst_of(last), ssem(len(chunks)), rsem(len(chunks)), where).start()

    send_slices(lambda part: proj_hbm.at[:, :, part], lambda part: p_buf.at[:, beta, :, part], p_chunks, lambda i: psend.at[i], lambda i: precv.at[i])
    for h, (g0, gn, chunks) in enumerate(phases):
        send_slices(lambda part: psi_hbm.at[:, pl.ds(g0, gn), :, part], lambda part: psi_buf.at[:, pl.ds(g0, gn), me_s, :, part],
                    chunks, lambda i: ssend.at[h, i], lambda i: srecv.at[h, i])

    lane = lax.broadcasted_iota(jnp.int32, (1, LANE), 1)
    small[0].wait()
    n_g = occ_buf.shape[1]
    occ_row[:, : occ_in.shape[1]] = occ_in[...]
    raw = occ_row[...]
    mine8 = (lane >= me_s * 8) & (lane < me_s * 8 + 8)
    for g in range(n_g):
        occ_buf[me_s, g : g + 1, :] = jnp.where(mine8, pltpu.roll(raw, me_s * 8 + (LANE - 8 * g) % LANE, 1), 0.0)
    for o in s_peers:
        remote(occ_buf.at[me_s], occ_buf.at[me_s], osend, orecv, number(o)).start()

    mine = local_copies(0, nt)
    more = local_copies(nt, 1)
    mine[0].wait()
    if_extra(lambda: more[0].wait())

    def clear(at, size):
        mil_buf[:, pl.ds(at, size)] = jnp.zeros((3, size), jnp.int32)
        psi_buf[:, :, :, :, pl.ds(at, size)] = jnp.zeros((*psi_buf.shape[:4], size), BF16)
        p_buf[:, :, :, pl.ds(at, size)] = jnp.zeros((2, na, PROJ, size), BF16)

    clear((nt + 1) * LANE, kp - (nt + 1) * LANE)

    @pl.when(jnp.logical_not(extra(me_s)))
    def _():
        clear(nt * LANE, LANE)

    small[1].wait()
    idx = [mil_buf[a : a + 1, :].astype(F32) for a in range(3)]
    co = [(idx[0] * lat_ref[0, a] + idx[1] * lat_ref[1, a] + idx[2] * lat_ref[2, a]) / MILLER for a in range(3)]
    iso = (co[0] * co[0] + co[1] * co[1] + co[2] * co[2]) / 3.0
    rows = list(co)
    for a, b in STRESS:
        prod = co[a] * co[b]
        rows.append(prod - iso if a == b else prod)
    for m, row in enumerate(rows):
        w_buf[m : m + 1, :] = row
    facc[...] = jnp.zeros_like(facc)
    sacc[...] = jnp.zeros_like(sacc)

    mine[1].wait()
    if_extra(lambda: more[1].wait())
    n_pc = len(p_chunks)
    up, down = number((1, 0, 0, 0, 0)), number((nz - 1, 0, 0, 0, 0))

    def plane(k):
        return pl.ds(pl.multiple_of(digits[0][k % nz] // n_r * n_s, n_s), n_s)

    def z_own(part, i):
        wait_recv(p_buf.at[:, pl.ds(0, n_s - 1), :, part], precv.at[i])
        ref = p_buf.at[:, plane(0), :, part]
        remote(ref, ref, zsend.at[0, i], zrecv.at[0, i], up).start()
        remote(ref, ref, zsend.at[1, i], zrecv.at[1, i], down).start()

    def z_next(part, i):
        wait_recv(p_buf.at[:, plane(0), :, part], zrecv.at[0, i])
        ref = p_buf.at[0, plane(-1), :, part]
        remote(ref, ref, zsend.at[2, i], zrecv.at[2, i], up).start()
        wait_recv(p_buf.at[:, plane(0), :, part], zrecv.at[1, i])
        ref = p_buf.at[1, plane(1), :, part]
        remote(ref, ref, zsend.at[3, i], zrecv.at[3, i], down).start()

    def z_end(part, i):
        wait_recv(p_buf.at[0, plane(0), :, part], zrecv.at[2, i])
        wait_recv(p_buf.at[1, plane(0), :, part], zrecv.at[3, i])

    def each_chunk(step):
        for i, chunk in enumerate(p_chunks):
            step(cols(chunk), i)
            if i == 0:
                if_extra(lambda: step(last, n_pc))

    each_chunk(z_own)
    each_chunk(z_next)

    mine[2].wait()
    if_extra(lambda: more[2].wait())
    for cp in small[2:]:
        cp.wait()
    kind = spec_ref[me_r]
    count = cnt_ref[me_r]
    act = (lax.broadcasted_iota(jnp.int32, (PROJ, PROJ), 0) < count) & (lax.broadcasted_iota(jnp.int32, (PROJ, PROJ), 1) < count)
    mat = jnp.where(act, coup_ref[kind], 0.0)
    front = lane < HALF
    z_done = [-1]

    def z_arrived(upto):
        while z_done[0] < n_pc - 1 and (z_done[0] < 0 or sum(p_chunks[z_done[0]]) < upto):
            z_done[0] += 1
            i = z_done[0]
            with jax.named_scope(f"wz{i}"):
                z_end(cols(p_chunks[i]), i)
            if i == 0:
                if_extra(lambda: z_end(last, n_pc))

    def gather_chunk(h, i):
        g0, gn, chunks = phases[h]
        acc = per[h][0]
        z_arrived(sum(chunks[i]))
        with jax.named_scope(f"wpsi{h}{i}"):
            wait_recv(psi_buf.at[:, pl.ds(g0, gn), pl.ds(0, n_s - 1), :, cols(chunks[i])], srecv.at[h, i])
        parts = [cols(chunks[i])]
        if i == 0:
            if_extra(lambda: wait_recv(psi_buf.at[:, pl.ds(g0, gn), pl.ds(0, n_s - 1), :, last], srecv.at[h, len(chunks)]))
            parts.append(pl.ds(nt * LANE, kp - nt * LANE))
        total = None if i == 0 else acc[...]
        for part in parts:
            rhs = jnp.concatenate([psi_buf[r, g, :, :, part].reshape(HALF, part.size) for g in range(g0, g0 + gn) for r in range(2)], axis=0)
            lhs = p_buf[:, :, :, part].reshape(2 * np_, part.size)
            term = lax.dot_general(lhs, rhs, (((1,), (1,)), ((), ())), preferred_element_type=F32)
            total = term if total is None else total + term
        acc[...] = total

    def reduce_start(h):
        acc, b_send, rs_buf = per[h][:3]
        for g in range(phases[h][1]):
            tile = pl.ds(g * LANE, LANE)
            low = pltpu.roll(acc[np_:, tile], HALF, 1)
            b_send[:, :, tile] = (acc[:np_, tile] + jnp.where(front, low, -low)).reshape(na, PROJ, LANE)
        for o in r_peers:
            remote(b_send.at[number(o) - base], rs_buf.at[me_r], rsend.at[h], rrecv.at[h], number(o)).start()
        rs_buf[me_r] = b_send[me_r]

    def mix_and_spread(h):
        rs_buf, uv_buf = per[h][2:4]
        if h == 0:
            wait_recv(occ_buf.at[pl.ds(0, n_s - 1)], orecv)
        with jax.named_scope(f"rs_wait{h}"):
            wait_recv(rs_buf.at[pl.ds(0, n_r - 1)], rrecv.at[h])
        total = jnp.sum(rs_buf[...], axis=0)
        mixed = jnp.zeros_like(total)
        for i in range(PROJ):
            mixed = mixed + mat[:, i : i + 1] * total[i : i + 1, :]
        occ = jnp.sum(occ_buf[...], axis=0)
        occ = occ + pltpu.roll(occ, HALF, 1)
        for g in range(phases[h][1]):
            tile = pl.ds(g * LANE, LANE)
            at = phases[h][0] + g
            uv_buf[me_r, :, tile] = (mixed[:, g * LANE : (g + 1) * LANE] * occ[at : at + 1, :]).astype(BF16)
        for o in r_peers:
            remote(uv_buf.at[me_r], uv_buf.at[me_r], asend.at[h], arecv.at[h], number(o)).start()

    def collect(h):
        uv_buf, left = per[h][3:5]
        with jax.named_scope(f"ag_wait{h}"):
            wait_recv(uv_buf.at[pl.ds(0, n_r - 1)], arecv.at[h])
        uv = uv_buf[...].reshape(np_, phases[h][1] * LANE)
        left[:np_] = uv
        for g in range(phases[h][1]):
            tile = pl.ds(g * LANE, LANE)
            turned = pltpu.roll(uv[:, g * LANE : (g + 1) * LANE].astype(F32), HALF, 1)
            left[np_:, tile] = jnp.where(front, -turned, turned).astype(BF16)

    wide = 256

    def weighted(h, i):
        g0, gn, _ = phases[h]
        part = pl.ds(pl.multiple_of(i * wide, wide), wide)
        rhs = jnp.concatenate([psi_buf[r, g, :, :, part].reshape(HALF, wide) for g in range(g0, g0 + gn) for r in range(2)], axis=0)
        return part, jnp.dot(per[h][4][...], rhs, preferred_element_type=F32)

    def block(h, i, carry):
        part, y = weighted(h, i)
        y_re, y_im = y[:np_], y[np_:]
        p_re, p_im = p_wide[0, :, part], p_wide[1, :, part]
        e_im = (p_re * y_im - p_im * y_re).reshape(na, PROJ, wide)
        e_re = jnp.sum((p_re * y_re + p_im * y_im).reshape(na, PROJ, wide), axis=0)
        for a in range(3):
            t = e_im * w_buf[a : a + 1, part].reshape(1, 1, wide)
            facc[a] += t[:, :, :LANE] + t[:, :, LANE:]
        for m in range(6):
            t = e_re * w_buf[3 + m : 4 + m, part]
            sacc[m] += t[:, :LANE] + t[:, LANE:]
        return carry

    for i in range(len(phases[0][2])):
        gather_chunk(0, i)
    reduce_start(0)
    p_wide[...] = p_buf[...].reshape(2, np_, kp).astype(F32)
    if n_ph > 1:
        for i in range(len(phases[1][2])):
            gather_chunk(1, i)
        reduce_start(1)
        mix_and_spread(0)
    mix_and_spread(n_ph - 1)
    if n_ph > 1:
        collect(0)
        lax.fori_loop(0, kp // wide, functools.partial(block, 0), 0, unroll=UNROLL)
    collect(n_ph - 1)
    lax.fori_loop(0, kp // wide, functools.partial(block, n_ph - 1), 0, unroll=UNROLL)

    row = jnp.zeros((1, LANE), F32)
    for a in range(3):
        f = jnp.sum(facc[a], axis=1)
        f = jnp.concatenate([jnp.zeros((a * na, LANE), F32), f, jnp.zeros((LANE - (a + 1) * na, LANE), F32)][0 if a else 1 :], axis=0)
        row = row + jnp.sum(f.T, axis=0, keepdims=True)
    for m in range(6):
        row = row + jnp.where(lane == 3 * na + m, jnp.sum(sacc[m], keepdims=True), 0.0)
    tot[me] = row
    for o in all_peers:
        remote(tot.at[me], tot.at[me], fsend, frecv, number(o)).start()
    wait_recv(tot.at[pl.ds(0, n_all - 1)], frecv)
    out_ref[...] = jnp.sum(tot[...], axis=0)

    for i, chunk in enumerate(p_chunks):
        wait_send(p_buf.at[:, pl.ds(0, n_s - 1), :, cols(chunk)], psend.at[i])

    def z_sent(part, i):
        for k in range(4):
            wait_send(p_buf.at[:, plane(0), :, part] if k < 2 else p_buf.at[0, plane(0), :, part], zsend.at[k, i])

    each_chunk(z_sent)
    for h, (g0, gn, chunks) in enumerate(phases):
        for i, chunk in enumerate(chunks):
            wait_send(psi_buf.at[:, pl.ds(g0, gn), pl.ds(0, n_s - 1), :, cols(chunk)], ssend.at[h, i])
        wait_send(per[h][2].at[pl.ds(0, n_r - 1)], rsend.at[h])
        wait_send(per[h][3].at[pl.ds(0, n_r - 1)], asend.at[h])
    for o in s_peers:

        @pl.when(extra(slice_of(o)))
        def _():
            wait_send(p_buf.at[:, 0, :, last], psend.at[n_pc])
            for h, (g0, gn, chunks) in enumerate(phases):
                wait_send(psi_buf.at[:, pl.ds(g0, gn), 0, :, last], ssend.at[h, len(chunks)])

    wait_send(occ_buf.at[pl.ds(0, n_s - 1)], osend)
    wait_send(tot.at[pl.ds(0, n_all - 1)], fsend)


def finish(dims, na, scales, row_ref, force_ref, stress_ref):
    res = row_ref[...]
    beta = (lax.axis_index("z") * dims[1] + lax.axis_index("yh")) * dims[2] + lax.axis_index("x")
    lane = lax.broadcasted_iota(jnp.int32, (1, LANE), 1)
    own = [jnp.sum(jnp.where(lane == a * na + beta, res, 0.0), axis=1, keepdims=True) for a in range(3)]
    force_ref[...] = jnp.where(lane[:, :3] == 0, own[0], jnp.where(lane[:, :3] == 1, own[1], own[2])) * scales[0]
    i0 = lax.broadcasted_iota(jnp.int32, (3, 3), 0)
    i1 = lax.broadcasted_iota(jnp.int32, (3, 3), 1)
    st = jnp.zeros((3, 3), F32)
    for m, (a, b) in enumerate(STRESS):
        val = jnp.sum(jnp.where(lane == 3 * na + m, res, 0.0), axis=1, keepdims=True)
        hit = ((i0 == a) & (i1 == b)) | ((i0 == b) & (i1 == a))
        st = st + jnp.where(hit, val, 0.0)
    stress_ref[...] = st * scales[1]


def cut(total, wants):
    chunks, at = [], 0
    for n in wants:
        if at + n < total:
            chunks.append((at, n))
            at += n
    chunks.append((at, total - at))
    return tuple(chunks)


UNROLL = 10
P_CUT = (4, 6)
SETS = ((2, (10,)), (2, (8, 8)))


def body(dims, psi, proj, miller, lattice, occupation, species, proj_count, coupling):
    nz, nyh, nx, nyl, nc = dims
    n_s = nyh * nx
    n_r = n_s * nyl * nc
    bands = psi.shape[1]
    n_g = bands // 8
    tiles = psi.shape[2] // LANE
    atoms = species.shape[0]
    nt = tiles // n_s
    p_chunks = cut(nt, P_CUT)
    phases, at = [], 0
    for gn, wants in SETS:
        phases.append((at, gn, cut(nt, wants)))
        at += gn
    n_ph = len(phases)
    most = max(len(chunks) for _, _, chunks in phases) + 1
    n_pc = len(p_chunks) + 1
    kp = -(-(nt + 1) * LANE // 256) * 256
    band_total = bands * n_s * nz
    scales = (2.0 / (PROJ * math.sqrt(band_total)), 1.0 / (PROJ * math.sqrt(atoms * band_total)))
    any_spec = pl.BlockSpec(memory_space=pl.ANY)
    vmem = pl.BlockSpec(memory_space=pltpu.VMEM)
    dma = pltpu.SemaphoreType.DMA
    scratch = [
        pltpu.VMEM((2, n_g, n_s, 8, kp), BF16),
        pltpu.VMEM((2, atoms, PROJ, kp), BF16),
        pltpu.VMEM((3, kp), jnp.int32),
        pltpu.VMEM((n_s, n_g, LANE), F32),
        pltpu.VMEM((16, kp), F32),
        pltpu.SMEM((3, 3), F32), pltpu.SMEM(species.shape, jnp.int32), pltpu.SMEM(species.shape, jnp.int32),
        pltpu.VMEM(coupling.shape, F32), pltpu.VMEM((1, LANE), F32), pltpu.VMEM((1, bands), F32),
        pltpu.VMEM((2, atoms * PROJ, kp), F32),
        pltpu.VMEM((3, atoms, PROJ, LANE), F32),
        pltpu.VMEM((6, PROJ, LANE), F32),
        pltpu.VMEM((nz * n_r, 1, LANE), F32),
    ]
    for _, gn, _ in phases:
        width = gn * LANE
        scratch += [
            pltpu.VMEM((2 * atoms * PROJ, width), F32),
            pltpu.VMEM((atoms, PROJ, width), F32),
            pltpu.VMEM((n_r, PROJ, width), F32),
            pltpu.VMEM((n_r, PROJ, width), BF16),
            pltpu.VMEM((2 * atoms * PROJ, width), BF16),
            ]
    scratch += [dma((8,)), *[dma((n_pc,))] * 2, *[dma((4, n_pc))] * 2, dma, dma, *[dma((n_ph, most))] * 2, *[dma((n_ph,))] * 4, dma, dma]
    row = pl.pallas_call(
        functools.partial(kernel, dims, nt, tiles, p_chunks, tuple(phases)),
        out_shape=pltpu.VMEM((1, LANE), F32),
        in_specs=[any_spec] * 8,
        out_specs=vmem,
        scratch_shapes=scratch,
        compiler_params=pltpu.CompilerParams(collective_id=0, has_side_effects=True, vmem_limit_bytes=58 << 20),
        name="plane_kernel",
    )(psi.reshape(2, n_g, 8, psi.shape[2]), proj, miller, lattice, occupation[None], species, proj_count, coupling)
    force, stress = pl.pallas_call(
        functools.partial(finish, dims, atoms, scales),
        out_shape=(jax.ShapeDtypeStruct((1, 3), F32), jax.ShapeDtypeStruct((3, 3), F32)),
        in_specs=[vmem],
        out_specs=(vmem, vmem),
        name="finish",
    )(pltpu.with_memory_space_constraint(row, pltpu.VMEM))
    return force.T, stress


def solution(mesh, dims=(4, 2, 4, 2, 2)):
    finer = Mesh(mesh.devices.reshape(dims), AXES)
    band, gvec = ("z", "yh", "x"), ("yl", "core")
    in_specs = (P(None, band, gvec), P(None, band, gvec), P(None, gvec), P(), P(band), P(), P(), P())
    return jax.shard_map(functools.partial(body, dims), mesh=finer, in_specs=in_specs, out_specs=(P(None, band), P()), check_vma=False)
```
